32 devices in a mesh: grp: 2 (over y), node: 4 (over z), head: 4 (over x, core).
Axes of the slice: x: 2, y: 2, z: 4, core: 2. Of those that a mesh axis runs over, the one named last changes fastest.
Arguments:
- q_nope: bfloat16 [512, 8192], P(('grp', 'node'), 'head'), parts along dimension 0, may hold values from -400 to 400
- q_rope: bfloat16 [512, 4096], P(('grp', 'node'), 'head'), parts along dimension 0, may hold values from -6 to 6
- kv_new: bfloat16 [512, 576], P(('grp', 'node')), parts along dimension 0, may hold values from -6 to 6
- kv_gain: float32 [512], replicated, may hold values from 0.5 to 1.5
- cache: bfloat16 [192, 64, 576], P(('grp', 'node')), parts along dimension 0, may hold values from -6 to 6
- w_uk: bfloat16 [64, 128, 512], P('head', 'node'), may hold values from -0.5 to 0.5
- w_uv: bfloat16 [64, 512, 128], P('head', 'node'), may hold values from -1 to 1
- hit_pages: int32 [8, 4], P('grp'), parts along dimension 0, may hold values from 0 to 95, as said below
- hit_len: int32 [8], P('grp'), parts along dimension 0, may hold values from 1 to 256
- page_slots: int32 [8, 1], P('grp'), parts along dimension 0, may hold values from 0 to 95, as said below
Outputs:
- attn_out: bfloat16 [512, 8192], P(('grp', 'node'), 'head'), parts along dimension 0
- new_cache: bfloat16 [192, 64, 576], P(('grp', 'node')), parts along dimension 0
The draws below stay inside these ranges and needn't reach their ends.
There are 2 independent parts, one for each index of `grp`. The reference program is written for one: setup_inputs(seed, part) draws one part's arguments, and reference() takes and returns one part's arrays. A program takes and returns all parts, laid end to end along the dimension named above; an argument that names none is the same for every part. Nothing has to cross between parts.
Inputs may be any that keep to these rules, and one draw needn't show every extreme that they name: `hit_pages`: page id = owner * 24 + local page; the owners named in one row are distinct. `page_slots`: page id = owner * 24 + local page; page p of session n lies with owner (n + p + 1) mod 4; no page is named twice.
All inputs are finite; a program needn't handle non-finite values.
Results may differ from the reference program's by a relative error of at most 0.012.
The reference program's roundings to bfloat16 on the way (of `new_pages`, `q_latent`, `q_pos`, `key_rows`, `weights` and `latent_out`) count: a program that leaves them out, or rounds other values in their place, can miss the bound.
Values may be sent and summed in bfloat16 or wider, within the bound.
A program may use at most 128 MiB of HBM per device.

```python
import math
import jax
import jax.numpy as jnp
from jax import lax

HEADS = 64
LATENT = 512
ROPE = 64
NOPE = 128
VHEAD = 128
BLOCK = 64
NEW = 64
BLK_DEV = 24
HITS = 4
PAGES = 1
TOKENS = 256
POOL = 96
N_NODE = 4


def draw_q_nope(key, part):
    values = jax.random.normal(key, (TOKENS, HEADS * NOPE), jnp.float32)
    values = jnp.clip(values, -6.0, 6.0)
    return values.astype(jnp.bfloat16)


def draw_hit_pages(key, part):
    row_keys = jax.random.split(key, N_NODE)

    def one_row(row_key):
        return jax.random.permutation(row_key, N_NODE)[:HITS]
    owners = jax.vmap(one_row)(row_keys).astype(jnp.int32)
    local_pages = jax.random.randint(jax.random.fold_in(key, 7), (N_NODE, HITS), 0, BLK_DEV)
    return (owners * BLK_DEV + local_pages).astype(jnp.int32)


def draw_hit_len(key, part):
    lengths = jax.random.randint(key, (N_NODE,), 1, HITS * BLOCK + 1)
    longest = jax.random.randint(jax.random.fold_in(key, 3), (), 0, N_NODE)
    lengths = jnp.where(jnp.arange(N_NODE) == longest, HITS * BLOCK, lengths)
    return lengths.astype(jnp.int32)


def draw_page_slots(key, part):
    start_slot = jax.random.randint(jax.random.fold_in(key, 3), (N_NODE,), 0, BLK_DEV)
    owner_ids = jnp.arange(N_NODE, dtype=jnp.int32)
    start_slot = jnp.where(owner_ids == 0, 0, start_slot)
    start_slot = jnp.where(owner_ids == N_NODE - 1, BLK_DEV - PAGES, start_slot)
    level = jnp.arange(PAGES, dtype=jnp.int32)
    sessions = jnp.arange(N_NODE, dtype=jnp.int32)
    owners = (sessions[:, None] + level[None, :] + 1) % N_NODE
    local_pages = (start_slot[owners] + level[None, :]) % BLK_DEV
    return (owners * BLK_DEV + local_pages).astype(jnp.int32)


def shard_levels(rng, dims, cuts, smallest, top_value):
    def one(axis_at, blocks):
        steps = jax.random.uniform(jax.random.fold_in(jax.random.fold_in(rng, 6), axis_at), (blocks,), jnp.float32, smallest / len(cuts), top_value / len(cuts))
        return jnp.repeat(jnp.exp(steps), dims[axis_at] // blocks).reshape((-1,) + (1,) * (len(dims) - axis_at - 1))

    gain = one(*cuts[0])
    for cut in cuts[1:]:
        gain = gain * one(*cut)
    return gain


def scatter_about(rng, shape, deviation, most, pieces=(), kind=jnp.bfloat16):
    entries = deviation * jax.random.normal(rng, shape, jnp.float32)
    if pieces:
        entries = entries * shard_levels(rng, shape, pieces, -0.22, 0.18)
    return jnp.clip(entries, -most, most).astype(kind)


def setup_inputs(seed: int = 0, part: int = 0) -> dict:
    key_of = jax.random.split(jax.random.key(seed), 11)
    own_keys = jax.random.split(jax.random.fold_in(key_of[10], part), 11)
    q_nope = draw_q_nope(jax.random.fold_in(jax.random.fold_in(key_of[10], part), 71), part)
    q_rope = scatter_about(own_keys[1], (TOKENS, HEADS * ROPE), 1.0, 6.0, ((0, 4), (1, 4)))
    kv_new = scatter_about(own_keys[2], (TOKENS, LATENT + ROPE), 1.0, 6.0, ((0, 4),))
    kv_gain = jnp.clip(1.0 + 0.1 * jax.random.normal(key_of[3], (LATENT,), jnp.float32), 0.5, 1.5)
    cache = scatter_about(own_keys[4], (POOL, BLOCK, LATENT + ROPE), 1.0, 6.0, ((0, 4),))
    w_uk = scatter_about(key_of[5], (HEADS, NOPE, LATENT), NOPE ** -0.5, 0.5, ((0, 4), (1, 4)))
    w_uv = scatter_about(key_of[6], (HEADS, LATENT, VHEAD), 0.18, 1.0, ((0, 4), (1, 4)))
    hit_pages = draw_hit_pages(jax.random.fold_in(jax.random.fold_in(key_of[10], part), 71), part)
    hit_len = draw_hit_len(jax.random.fold_in(jax.random.fold_in(key_of[10], part), 71), part)
    page_slots = draw_page_slots(jax.random.fold_in(jax.random.fold_in(key_of[10], part), 71), part)
    return {"q_nope": q_nope, "q_rope": q_rope, "kv_new": kv_new, "kv_gain": kv_gain, "cache": cache, "w_uk": w_uk, "w_uv": w_uv, "hit_pages": hit_pages, "hit_len": hit_len, "page_slots": page_slots}


def rotate(values, position):
    half_rope = ROPE // 2
    inverse = 10000.0 ** (-(jnp.arange(half_rope, dtype=jnp.float32) * 2.0 / ROPE))
    angles = position.astype(jnp.float32)[..., None] * inverse
    first_half = values[..., :half_rope]
    second_half = values[..., half_rope:]
    cosine = jnp.cos(angles)
    sine = jnp.sin(angles)
    return jnp.concatenate([first_half * cosine - second_half * sine, first_half * sine + second_half * cosine], axis=-1)

def make_pages(kv_rows, kv_gain, offset):
    latent = kv_rows[:, :LATENT].astype(jnp.float32)
    normed = latent * lax.rsqrt(lax.optimization_barrier(jnp.mean(latent * latent, axis=-1, keepdims=True)) + 1e-06) * kv_gain
    rotary = rotate(kv_rows[:, LATENT:].astype(jnp.float32), offset + jnp.arange(kv_rows.shape[0], dtype=jnp.int32))
    return jnp.concatenate([normed, rotary], axis=-1).astype(jnp.bfloat16)

def reference(q_nope, q_rope, kv_new, kv_gain, cache, w_uk, w_uv, hit_pages, hit_len, page_slots):
    score_scale = 1.0 / math.sqrt(NOPE + ROPE)
    width = LATENT + ROPE
    kv_sessions = kv_new.reshape(N_NODE, NEW, width)
    new_pages = jax.vmap(make_pages, in_axes=(0, None, 0))(kv_sessions, kv_gain, hit_len)
    new_index = jnp.arange(NEW, dtype=jnp.int32)
    causal = new_index[None, :] <= new_index[:, None]

    def session(number):
        q_rows = lax.dynamic_slice_in_dim(q_nope, number * NEW, NEW, 0).reshape(NEW, HEADS, NOPE)
        r_rows = lax.dynamic_slice_in_dim(q_rope, number * NEW, NEW, 0).reshape(NEW, HEADS, ROPE)
        offset = hit_len[number]
        q_latent = jnp.einsum('thk,hkc->thc', q_rows.astype(jnp.float32), w_uk.astype(jnp.float32)).astype(jnp.bfloat16)
        q_pos = rotate(r_rows.astype(jnp.float32), (offset + new_index)[:, None]).astype(jnp.bfloat16)
        prefix = cache[hit_pages[number]].reshape(HITS * BLOCK, width)
        key_rows = jnp.concatenate([prefix, new_pages[number]], axis=0)
        prefix_seen = jnp.arange(HITS * BLOCK, dtype=jnp.int32) < offset
        visible = jnp.concatenate([jnp.broadcast_to(prefix_seen[None, :], (NEW, HITS * BLOCK)), causal], axis=1)
        key_latent = key_rows[:, :LATENT].astype(jnp.float32)
        key_rotary = key_rows[:, LATENT:].astype(jnp.float32)
        scores = jnp.einsum('thc,kc->thk', q_latent.astype(jnp.float32), key_latent)
        scores = (scores + jnp.einsum('thr,kr->thk', q_pos.astype(jnp.float32), key_rotary)) * score_scale
        scores = jnp.where(visible[:, None, :], scores, -1e+30)
        row_max = lax.optimization_barrier(jnp.max(scores, axis=-1, keepdims=True))
        expo_terms = jnp.where(visible[:, None, :], jnp.exp(scores - row_max), 0.0)
        weights = (expo_terms / lax.optimization_barrier(jnp.sum(expo_terms, axis=-1, keepdims=True))).astype(jnp.bfloat16)
        latent_out = jnp.einsum('thk,kc->thc', weights.astype(jnp.float32), key_latent).astype(jnp.bfloat16)
        result = jnp.einsum('thc,hcv->thv', latent_out.astype(jnp.float32), w_uv.astype(jnp.float32))
        return result.astype(jnp.bfloat16).reshape(NEW, HEADS * VHEAD)
    attn_out = lax.map(session, jnp.arange(N_NODE, dtype=jnp.int32)).reshape(TOKENS, HEADS * VHEAD)
    new_cache = cache.at[page_slots.reshape(-1)].set(new_pages.reshape(N_NODE * PAGES, BLOCK, width))
    return (attn_out, new_cache)
```

```python
import functools
import math

import jax
import jax.numpy as jnp
from jax import lax
from jax.experimental import pallas as pl
from jax.experimental.pallas import tpu as pltpu
from jax.sharding import PartitionSpec as P

LATENT = 512
ROPE = 64
NOPE = 128
VHEAD = 128
BLOCK = 64
NEW = 64
BLK_DEV = 24
PHASES_K = 1
PHASES_V = 1
MESH = pl.DeviceIdType.MESH


def from_behind(block, axis, distance):
    devices = range(lax.axis_size(axis))
    route = [((i - distance) % len(devices), i) for i in devices]
    return lax.ppermute(block, axis, route)


def rotate(values, position):
    half_rope = ROPE // 2
    inverse = 10000.0 ** (-(jnp.arange(half_rope, dtype=jnp.float32) * 2.0 / ROPE))
    angles = position.astype(jnp.float32)[..., None] * inverse
    first_half = values[..., :half_rope]
    second_half = values[..., half_rope:]
    cosine = jnp.cos(angles)
    sine = jnp.sin(angles)
    return jnp.concatenate(
        [first_half * cosine - second_half * sine, first_half * sine + second_half * cosine],
        axis=-1,
    )


def make_pages(kv_rows, kv_gain, offset):
    latent = kv_rows[:, :LATENT].astype(jnp.float32)
    normed = latent * lax.rsqrt(jnp.mean(latent * latent, axis=-1, keepdims=True) + 1e-06) * kv_gain
    rotary = rotate(
        kv_rows[:, LATENT:].astype(jnp.float32),
        offset + jnp.arange(kv_rows.shape[0], dtype=jnp.int32),
    )
    return jnp.concatenate([normed, rotary], axis=-1).astype(jnp.bfloat16)


def select_rows(selector, blocks):
    flat = blocks.reshape(blocks.shape[0], -1)
    picked = jnp.dot(selector, flat, preferred_element_type=jnp.float32).astype(jnp.bfloat16)
    return picked.reshape((selector.shape[0],) + blocks.shape[1:])


def per_device(q_nope, q_rope, kv_new, kv_gain, cache, w_uk, w_uv, hit_pages, hit_len, page_slots):
    this_node = lax.axis_index("node")
    nodes = lax.axis_size("node")
    width = LATENT + ROPE
    heads_local = w_uk.shape[0]
    hits = hit_pages.shape[1]
    pages_each = NEW // BLOCK
    score_scale = 1.0 / math.sqrt(NOPE + ROPE)
    node_ids = jnp.arange(nodes, dtype=jnp.int32)
    new_index = jnp.arange(NEW, dtype=jnp.int32)
    offset = hit_len[this_node]
    new_pages = make_pages(kv_new, kv_gain, offset)
    page_blocks = new_pages.reshape(pages_each, BLOCK, width)
    own_pages = this_node * BLK_DEV + jnp.arange(BLK_DEV, dtype=jnp.int32)
    wanted = jnp.sum(
        (hit_pages[:, :, None] == own_pages[None, None, :]).astype(jnp.int32), axis=1
    ).astype(jnp.bfloat16)
    order_pick = ((hit_pages[this_node] // BLK_DEV)[:, None] == node_ids[None, :]).astype(
        jnp.bfloat16
    )
    columns = width // lax.axis_size("head")
    cache_part = lax.dynamic_slice_in_dim(cache, lax.axis_index("head") * columns, columns, 2)
    pulled = lax.all_to_all(
        select_rows(wanted, cache_part), "node", split_axis=0, concat_axis=0, tiled=True
    )
    prefix = select_rows(order_pick, pulled)
    prefix = lax.all_gather(prefix, "head", axis=2, tiled=True)
    q_rows = q_nope.reshape(NEW, heads_local, NOPE)
    q_pos = rotate(
        q_rope.reshape(NEW, heads_local, ROPE).astype(jnp.float32), (offset + new_index)[:, None]
    ).astype(jnp.bfloat16)
    q_pos = jnp.transpose(q_pos, (1, 0, 2))
    key_weight, value_weight = (
        lax.all_gather(w_uk, "node", axis=1, tiled=True),
        lax.all_gather(w_uv, "node", axis=1, tiled=True),
    )
    q_latent = jnp.einsum(
        "thk,hkc->htc", q_rows, key_weight, preferred_element_type=jnp.float32
    ).astype(jnp.bfloat16)
    key_rows = jnp.concatenate([prefix.reshape(hits * BLOCK, width), new_pages], axis=0)
    key_latent = key_rows[:, :LATENT]
    key_rotary = key_rows[:, LATENT:]
    prefix_seen = jnp.arange(hits * BLOCK, dtype=jnp.int32) < offset
    causal = new_index[None, :] <= new_index[:, None]
    visible = jnp.concatenate(
        [jnp.broadcast_to(prefix_seen[None, :], (NEW, hits * BLOCK)), causal], axis=1
    )
    target = max(1, 512 // NEW)
    group_size = 1
    for trial in range(1, heads_local + 1):
        if heads_local % trial == 0 and trial <= target:
            group_size = trial

    def attend(operands):
        q_part, r_part = operands
        scores = jnp.einsum("htc,kc->htk", q_part, key_latent, preferred_element_type=jnp.float32)
        scores = (
            scores
            + jnp.einsum("htr,kr->htk", r_part, key_rotary, preferred_element_type=jnp.float32)
        ) * score_scale
        scores = jnp.where(visible[None, :, :], scores, -1e30)
        row_max = jnp.max(scores, axis=-1, keepdims=True)
        expo_terms = jnp.where(visible[None, :, :], jnp.exp(scores - row_max), 0.0)
        weights = (expo_terms / jnp.sum(expo_terms, axis=-1, keepdims=True)).astype(jnp.bfloat16)
        return jnp.einsum(
            "htk,kc->htc", weights, key_latent, preferred_element_type=jnp.float32
        ).astype(jnp.bfloat16)

    groups = heads_local // group_size
    latent_out = lax.map(
        attend,
        (
            q_latent.reshape(groups, group_size, NEW, LATENT),
            q_pos.reshape(groups, group_size, NEW, ROPE),
        ),
    )
    latent_out = latent_out.reshape(heads_local, NEW, LATENT)
    projected = jnp.einsum(
        "htc,hcv->thv", latent_out, value_weight, preferred_element_type=jnp.float32
    )
    attn_out = projected.astype(jnp.bfloat16).reshape(NEW, heads_local * VHEAD)
    local_ids = jnp.arange(BLK_DEV, dtype=jnp.int32)
    new_cache = cache
    arrived = from_behind(page_blocks[0], "node", 1)
    sender = (this_node - 0 - 1 + nodes) % nodes
    slot = page_slots[sender, 0] - this_node * BLK_DEV
    new_cache = jnp.where((local_ids == slot)[:, None, None], arrived[None, :, :], new_cache)
    return (attn_out, new_cache)


def order(count):
    steps = []
    for near in range(1, count // 2 + 1):
        steps.append(near)
        if near != count - near:
            steps.append(count - near)
    return steps


def fused_kernel(
    nodes, grps, fan, phases_k, phases_v, score_scale,
    pages_in, len_in, slot_in, gain_in, qn_ref, qr_ref, kv_ref, cache_ref, uk_ref, uv_ref,
    attn_ref, CB,
    UK, UV, KB, PAY, KV, Q, QR, QP, QL, LAT, OUT, pages_ref, len_ref, slot_ref, gain_ref,
    zs_s, zs_r, f_s, f_r, q_s, q_r, k_s, k_r, wk_s, wk_r, yk_s, yk_r, wv_s, wv_r, yv_s, yv_r, loc, o_s, o_r,
):
    z = lax.axis_index("node")
    y = lax.axis_index("grp")
    hd = lax.axis_index("head")
    b = z % 2
    p = z // 2
    mate = z + 1 - 2 * b
    after = (z + 1) % nodes
    back = (z + nodes - 1) % nodes
    half = UK.shape[0]
    owned = cache_ref.shape[0]
    rows_k = uk_ref.shape[1]
    rows_v = uv_ref.shape[1]
    part = BLOCK // fan
    hits = pages_ref.shape[1]
    old = nodes * BLOCK
    steps = order(nodes)

    barrier = pltpu.get_barrier_semaphore()
    for k in range(1, nodes):
        pl.semaphore_signal(barrier, 1, device_id={"node": (z + k) % nodes}, device_id_type=MESH)
    for k in range(1, fan):
        pl.semaphore_signal(barrier, 1, device_id={"head": (hd + k) % fan}, device_id_type=MESH)
    pl.semaphore_signal(barrier, 1, device_id={"grp": 1 - y}, device_id_type=MESH)

    sends = []

    def remote(src, dst, send, recv, to):
        return pltpu.make_async_remote_copy(
            src_ref=src, dst_ref=dst, send_sem=send, recv_sem=recv, device_id=to, device_id_type=MESH
        )

    def go(*copy):
        copy = remote(*copy)
        copy.start()
        sends.append(copy)

    def arrive(block, send, recv, origin):
        remote(block, block, send, recv, origin).wait_recv()

    def key_part(node, head):
        at = pl.multiple_of(node * BLOCK + head * part, part)
        return KB.at[:, pl.ds(at, part), :]

    def kv_part(kind, head):
        return KV.at[kind, pl.ds(pl.multiple_of(head * part, part), part), :]

    mine = pl.ds(pl.multiple_of(b * NEW, NEW), NEW)
    theirs = pl.ds(pl.multiple_of((1 - b) * NEW, NEW), NEW)
    load = pltpu.make_async_copy(cache_ref, CB, loc.at[0])
    tables = [
        pltpu.make_async_copy(src, dst, loc.at[6 + i])
        for i, (src, dst) in enumerate(
            ((pages_in, pages_ref), (len_in, len_ref), (slot_in, slot_ref), (gain_in, gain_ref))
        )
    ]
    for copy in tables:
        copy.start()
    load.start()
    locals_ = [
        pltpu.make_async_copy(kv_ref, KV.at[2], loc.at[1]),
        pltpu.make_async_copy(uk_ref.at[pl.ds(b * half, half)], UK.at[:, pl.ds(pl.multiple_of(z * rows_k, rows_k), rows_k), :], loc.at[4]),
        pltpu.make_async_copy(uv_ref.at[pl.ds(b * half, half)], UV.at[:, pl.ds(pl.multiple_of(z * rows_v, rows_v), rows_v), :], loc.at[5]),
    ]
    for slot, (src, dst, wide) in enumerate(((qn_ref, Q, NOPE), (qr_ref, QR, ROPE))):
        cols = pl.ds(pl.multiple_of(b * half * wide, 128), half * wide)
        locals_.append(pltpu.make_async_copy(src.at[:, cols], dst.at[mine, :], loc.at[2 + slot]))
    for copy in locals_:
        copy.start()
    pl.semaphore_wait(barrier, nodes - 1 + fan - 1 + 1)

    kinds = (
        (uk_ref, UK, rows_k, phases_k, wk_s, wk_r, yk_s, yk_r),
        (uv_ref, UV, rows_v, phases_v, wv_s, wv_r, yv_s, yv_r),
    )

    def weight_part(kind, f, node, grp):
        buffer, rows, phases = kinds[kind][1:4]
        count = half // phases
        sub = count // grps
        return buffer.at[
            pl.ds(f * count + grp * sub, sub), pl.ds(pl.multiple_of(node * rows, rows), rows), :
        ]

    def send_weights(kind, f):
        src, _, _, phases, send, recv, _, _ = kinds[kind]
        count = half // phases
        sub = count // grps
        for k in steps:
            to = (z + k) % nodes
            rows = pl.ds((to % 2) * half + f * count + y * sub, sub)
            go(src.at[rows], weight_part(kind, f, z, y), send.at[f, k], recv.at[f, k], {"node": to})

    def pass_on(kind, f, which=steps):
        send, recv, over_s, over_r = kinds[kind][4:]
        for k in which:
            origin = (z + nodes - k) % nodes
            block = weight_part(kind, f, origin, y)
            arrive(block, send.at[f, k], recv.at[f, k], {"node": origin})
            go(block, block, over_s.at[f, k], over_r.at[f, k], {"grp": 1 - y})

    def take(kind, f):
        over_s, over_r = kinds[kind][6:]
        for k in steps:
            block = weight_part(kind, f, (z + nodes - k) % nodes, 1 - y)
            arrive(block, over_s.at[f, k], over_r.at[f, k], {"grp": 1 - y})

    quarter = pl.ds(pl.multiple_of(hd * part, part), part)
    send_weights(0, 0)
    for slot, (src, dst, wide) in enumerate(((qn_ref, Q, NOPE), (qr_ref, QR, ROPE))):
        cols = pl.ds(pl.multiple_of((1 - b) * half * wide, 128), half * wide)
        go(src.at[:, cols], dst.at[mine, :], q_s.at[slot], q_r.at[slot], {"node": mate})
    for kind, to in enumerate((mate, after)):
        go(kv_ref.at[quarter, :], kv_part(kind, hd), k_s.at[kind, 0], k_r.at[kind, 0], {"node": to})

    load.wait()
    for copy in tables:
        copy.wait()

    def local_page(session):
        local = jnp.int32(0)
        for j in range(hits):
            page = pages_ref[session, j] - z * owned
            local = jnp.where((page >= 0) & (page < owned), page, local)
        return local

    for n in range(nodes):
        PAY[n] = CB[local_page(n), quarter, :]
    for i in range(2):
        KB[i, pl.ds(pl.multiple_of(z * BLOCK, BLOCK), BLOCK), :] = CB[local_page(2 * p + i)]

    lane = lax.broadcasted_iota(jnp.int32, (1, 128), 1) % (ROPE // 2)
    freq = jnp.exp(lane.astype(jnp.float32) * (-2.0 * math.log(10000.0) / ROPE))

    def angles(session):
        at = (len_ref[session] + lax.broadcasted_iota(jnp.int32, (NEW, 128), 0)).astype(jnp.float32)
        turn = at * freq
        return jnp.cos(turn), jnp.sin(turn)

    turns = [angles(2 * p + i) for i in range(2)]
    turn_back = angles(back)
    for copy in locals_:
        copy.wait()

    def new_page(kind, cosine, sine):
        raw = KV[kind].astype(jnp.float32)
        latent = raw[:, :LATENT]
        mean = jnp.sum(latent * latent, axis=-1, keepdims=True) * (1.0 / LATENT)
        normed = latent * lax.rsqrt(mean + 1e-06) * gain_ref[...]
        rot = raw[:, LATENT:]
        swapped = jnp.concatenate([-rot[:, ROPE // 2:], rot[:, :ROPE // 2]], axis=-1)
        rotary = rot * cosine[:, :ROPE] + swapped * sine[:, :ROPE]
        return jnp.concatenate([normed, rotary], axis=-1).astype(jnp.bfloat16)

    KB[b, old:, :] = new_page(2, *[jnp.where(b == 0, t, u) for t, u in zip(*turns)])

    for k in steps:
        to = (z + k) % nodes
        go(
            PAY.at[pl.ds((to // 2) * 2, 2)], key_part(z, hd), zs_s.at[k], zs_r.at[k], {"node": to}
        )
    for f in range(1, phases_k):
        send_weights(0, f)
    for f in range(phases_v):
        send_weights(1, f)

    pass_on(0, 0)
    for slot, dst in enumerate((Q, QR)):
        arrive(dst.at[theirs, :], q_s.at[slot], q_r.at[slot], {"node": mate})
    for kind, origin in enumerate((mate, back)):
        block = kv_part(kind, hd)
        arrive(block, k_s.at[kind, 0], k_r.at[kind, 0], {"node": origin})
        for j in range(1, fan):
            go(block, block, k_s.at[kind, j], k_r.at[kind, j], {"head": (hd + j) % fan})
    for k in steps:
        origin = (z + nodes - k) % nodes
        block = key_part(origin, hd)
        arrive(block, zs_s.at[k], zs_r.at[k], {"node": origin})
        for j in range(1, fan):
            go(block, block, f_s.at[k, j], f_r.at[k, j], {"head": (hd + j) % fan})

    wide = half * ROPE
    first = (lax.broadcasted_iota(jnp.int32, (NEW, wide), 1) % ROPE) < ROPE // 2
    for i in range(2):
        cosine, sine = (jnp.concatenate([t] * (wide // 128), axis=1) for t in turns[i])
        x = QR[i * NEW:(i + 1) * NEW, :].astype(jnp.float32)
        ahead = pltpu.roll(x, wide - ROPE // 2, 1)
        behind = pltpu.roll(x, ROPE // 2, 1)
        turned = (x * cosine + jnp.where(first, -ahead, behind) * sine).astype(jnp.bfloat16)
        for h in range(half):
            QP[h, i * NEW:(i + 1) * NEW, :] = turned[:, h * ROPE:(h + 1) * ROPE]

    for kind in range(2):
        for j in range(1, fan):
            from_head = (hd + fan - j) % fan
            arrive(kv_part(kind, from_head), k_s.at[kind, j], k_r.at[kind, j], {"head": from_head})
    KB[1 - b, old:, :] = new_page(0, *[jnp.where(b == 0, u, t) for t, u in zip(*turns)])
    arrived = new_page(1, *turn_back)
    slot = slot_ref[0, back] - z * owned

    def place(n, carry):
        CB[n] = jnp.where(slot == n, arrived, CB[n])
        return carry

    lax.fori_loop(0, owned, place, 0)

    for k in steps:
        origin = (z + nodes - k) % nodes
        for j in range(1, fan):
            from_head = (hd + fan - j) % fan
            arrive(key_part(origin, from_head), f_s.at[k, j], f_r.at[k, j], {"head": from_head})

    contract_last = (((1,), (1,)), ((), ()))
    total = old + NEW
    column = lax.broadcasted_iota(jnp.int32, (NEW, total), 1)
    token = lax.broadcasted_iota(jnp.int32, (NEW, total), 0)
    group = half // phases_k

    def attend(f, i):
        session = 2 * p + i
        seen = (column >= old) & (column - old <= token)
        for j in range(hits):
            local = column - (pages_ref[session, j] // owned) * BLOCK
            limit = jnp.minimum(len_ref[session] - j * BLOCK, BLOCK)
            seen = seen | ((column < old) & (local >= 0) & (local < limit))
        key_latent = KB[i, :, :LATENT]
        key_rotary = KB[i, :, LATENT:]
        heads = slice(f * group, (f + 1) * group)
        tokens = slice(i * NEW, (i + 1) * NEW)
        q_part = QL[heads, tokens, :].reshape(group * NEW, LATENT)
        r_part = QP[heads, tokens, :].reshape(group * NEW, ROPE)
        scores = lax.dot_general(q_part, key_latent, contract_last, preferred_element_type=jnp.float32)
        scores = scores + lax.dot_general(r_part, key_rotary, contract_last, preferred_element_type=jnp.float32)
        scores = (scores * score_scale).reshape(group, NEW, total)
        scores = jnp.where(seen[None], scores, -1e30)
        row_max = jnp.max(scores, axis=-1, keepdims=True)
        terms = jnp.where(seen[None], jnp.exp(scores - row_max), 0.0)
        weights = (terms / jnp.sum(terms, axis=-1, keepdims=True)).astype(jnp.bfloat16)
        mixed = jnp.dot(
            weights.reshape(group * NEW, total), key_latent, preferred_element_type=jnp.float32
        ).astype(jnp.bfloat16)
        LAT[heads, tokens, :] = mixed.reshape(group, NEW, LATENT)

    for f in range(phases_k):
        if f > 0:
            pass_on(0, f)
        take(0, f)
        for h in range(f * group, (f + 1) * group):
            QL[h] = jnp.dot(
                Q[:, h * NOPE:(h + 1) * NOPE], UK[h], preferred_element_type=jnp.float32
            ).astype(jnp.bfloat16)
        attend(f, 0)
        if f == phases_k - 1:
            pass_on(1, 0, steps[:1])
        attend(f, 1)

    count = half // phases_v
    for f in range(phases_v):
        pass_on(1, f, steps if f > 0 else steps[1:])
        take(1, f)
        for h in range(f * count, (f + 1) * count):
            OUT[:, h * VHEAD:(h + 1) * VHEAD] = jnp.dot(
                LAT[h], UV[h], preferred_element_type=jnp.float32
            ).astype(jnp.bfloat16)
        here = pl.ds(f * count * VHEAD, count * VHEAD)
        there = pl.ds(pl.multiple_of((b * half + f * count) * VHEAD, 128), count * VHEAD)
        go(OUT.at[theirs, here], attn_ref.at[:, there], o_s.at[f], o_r.at[f], {"node": mate})
    cols = pl.ds(pl.multiple_of(b * half * VHEAD, 128), half * VHEAD)
    attn_ref[:, cols] = OUT[mine, :]
    for f in range(phases_v):
        there = pl.ds(pl.multiple_of(((1 - b) * half + f * count) * VHEAD, 128), count * VHEAD)
        block = attn_ref.at[:, there]
        arrive(block, o_s.at[f], o_r.at[f], {"node": mate})
    for copy in sends:
        copy.wait_send()


def write_kernel(attn_ref, pages_ref, attn_out, pages_out, done):
    copies = [
        pltpu.make_async_copy(attn_ref, attn_out, done.at[0]),
        pltpu.make_async_copy(pages_ref, pages_out, done.at[1]),
    ]
    for copy in copies:
        copy.start()
    for copy in copies:
        copy.wait()


def fused_device(q_nope, q_rope, kv_new, kv_gain, cache, w_uk, w_uv, hit_pages, hit_len, page_slots):
    nodes = lax.axis_size("node")
    grps = lax.axis_size("grp")
    fan = lax.axis_size("head")
    width = LATENT + ROPE
    owned = cache.shape[0]
    half = w_uk.shape[0] // 2
    phases_k = PHASES_K if half % (PHASES_K * grps) == 0 else 1
    phases_v = PHASES_V if half % (PHASES_V * grps) == 0 else 1
    vmem = pl.BlockSpec(memory_space=pltpu.VMEM)
    anywhere = pl.BlockSpec(memory_space=pl.ANY)
    bf16 = jnp.bfloat16
    dma = pltpu.SemaphoreType.DMA
    k_sem = dma((phases_k, nodes))
    v_sem = dma((phases_v, nodes))
    attn, pages = pl.pallas_call(
        functools.partial(
            fused_kernel, nodes, grps, fan, phases_k, phases_v, 1.0 / math.sqrt(NOPE + ROPE)
        ),
        name="fused",
        out_shape=(
            pltpu.VMEM((NEW, 2 * half * VHEAD), bf16),
            pltpu.VMEM(cache.shape, bf16),
        ),
        in_specs=[anywhere] * 10,
        out_specs=(vmem, vmem),
        scratch_shapes=[
            pltpu.VMEM((half, NOPE, LATENT), bf16),
            pltpu.VMEM((half, LATENT, VHEAD), bf16),
            pltpu.VMEM((2, nodes * BLOCK + NEW, width), bf16),
            pltpu.VMEM((nodes, BLOCK // fan, width), bf16),
            pltpu.VMEM((3, NEW, width), bf16),
            pltpu.VMEM((2 * NEW, half * NOPE), bf16),
            pltpu.VMEM((2 * NEW, half * ROPE), bf16),
            pltpu.VMEM((half, 2 * NEW, ROPE), bf16),
            pltpu.VMEM((half, 2 * NEW, LATENT), bf16),
            pltpu.VMEM((half, 2 * NEW, LATENT), bf16),
            pltpu.VMEM((2 * NEW, half * VHEAD), bf16),
            pltpu.SMEM(hit_pages.shape, jnp.int32),
            pltpu.SMEM(hit_len.shape, jnp.int32),
            pltpu.SMEM(page_slots.shape[::-1], jnp.int32),
            pltpu.VMEM((1, LATENT), jnp.float32),
            dma((nodes,)), dma((nodes,)), dma((nodes, fan)), dma((nodes, fan)), dma((2,)), dma((2,)),
            dma((2, fan)), dma((2, fan)), k_sem, k_sem, k_sem, k_sem, v_sem, v_sem, v_sem, v_sem,
            dma((10,)), dma((phases_v,)), dma((phases_v,)),
        ],
        compiler_params=pltpu.CompilerParams(
            collective_id=0, has_side_effects=True, vmem_limit_bytes=60 << 20
        ),
    )(hit_pages, hit_len, page_slots.T, kv_gain[None, :], q_nope, q_rope, kv_new, cache, w_uk, w_uv)
    return pl.pallas_call(
        write_kernel,
        name="write",
        out_shape=(
            jax.ShapeDtypeStruct(attn.shape, bf16),
            jax.ShapeDtypeStruct(cache.shape, bf16),
        ),
        in_specs=[vmem, vmem],
        out_specs=(anywhere, anywhere),
        scratch_shapes=[dma((2,))],
    )(*(pltpu.with_memory_space_constraint(x, pltpu.VMEM) for x in (attn, pages)))


def choose(*operands):
    w_uk, w_uv = operands[5], operands[6]
    nodes, grps, fan = (lax.axis_size(name) for name in ("node", "grp", "head"))
    fits = (
        nodes % 2 == 0
        and grps == 2
        and NEW == BLOCK
        and BLOCK % (16 * fan) == 0
        and w_uk.shape[0] % 4 == 0
        and w_uk.shape[1] % 16 == 0
        and w_uv.shape[1] % 16 == 0
    )
    return (fused_device if fits else per_device)(*operands)


def solution(mesh):
    placed = (
        P(("grp", "node"), "head"),
        P(("grp", "node"), "head"),
        P(("grp", "node"), None),
        P(),
        P(("grp", "node"), None, None),
        P("head", "node", None),
        P("head", "node", None),
        P("grp", None),
        P("grp"),
        P("grp", None),
    )
    return jax.shard_map(
        choose,
        mesh=mesh,
        in_specs=placed,
        out_specs=(P(("grp", "node"), "head"), P(("grp", "node"), None, None)),
        check_vma=False,
    )
```

```python
import functools
import math

import jax
import jax.numpy as jnp
from jax import lax
from jax.experimental import pallas as pl
from jax.experimental.pallas import tpu as pltpu
from jax.sharding import PartitionSpec as P

LATENT = 512
ROPE = 64
NOPE = 128
VHEAD = 128
BLOCK = 64
NEW = 64
BLK_DEV = 24
PHASES = 4
MESH = pl.DeviceIdType.MESH


def from_behind(block, axis, distance):
    devices = range(lax.axis_size(axis))
    route = [((i - distance) % len(devices), i) for i in devices]
    return lax.ppermute(block, axis, route)


def rotate(values, position):
    half_rope = ROPE // 2
    inverse = 10000.0 ** (-(jnp.arange(half_rope, dtype=jnp.float32) * 2.0 / ROPE))
    angles = position.astype(jnp.float32)[..., None] * inverse
    first_half = values[..., :half_rope]
    second_half = values[..., half_rope:]
    cosine = jnp.cos(angles)
    sine = jnp.sin(angles)
    return jnp.concatenate(
        [first_half * cosine - second_half * sine, first_half * sine + second_half * cosine],
        axis=-1,
    )


def make_pages(kv_rows, kv_gain, offset):
    latent = kv_rows[:, :LATENT].astype(jnp.float32)
    normed = latent * lax.rsqrt(jnp.mean(latent * latent, axis=-1, keepdims=True) + 1e-06) * kv_gain
    rotary = rotate(
        kv_rows[:, LATENT:].astype(jnp.float32),
        offset + jnp.arange(kv_rows.shape[0], dtype=jnp.int32),
    )
    return jnp.concatenate([normed, rotary], axis=-1).astype(jnp.bfloat16)


def select_rows(selector, blocks):
    flat = blocks.reshape(blocks.shape[0], -1)
    picked = jnp.dot(selector, flat, preferred_element_type=jnp.float32).astype(jnp.bfloat16)
    return picked.reshape((selector.shape[0],) + blocks.shape[1:])


def per_device(q_nope, q_rope, kv_new, kv_gain, cache, w_uk, w_uv, hit_pages, hit_len, page_slots):
    this_node = lax.axis_index("node")
    nodes = lax.axis_size("node")
    width = LATENT + ROPE
    heads_local = w_uk.shape[0]
    hits = hit_pages.shape[1]
    pages_each = NEW // BLOCK
    score_scale = 1.0 / math.sqrt(NOPE + ROPE)
    node_ids = jnp.arange(nodes, dtype=jnp.int32)
    new_index = jnp.arange(NEW, dtype=jnp.int32)
    offset = hit_len[this_node]
    new_pages = make_pages(kv_new, kv_gain, offset)
    page_blocks = new_pages.reshape(pages_each, BLOCK, width)
    own_pages = this_node * BLK_DEV + jnp.arange(BLK_DEV, dtype=jnp.int32)
    wanted = jnp.sum(
        (hit_pages[:, :, None] == own_pages[None, None, :]).astype(jnp.int32), axis=1
    ).astype(jnp.bfloat16)
    order_pick = ((hit_pages[this_node] // BLK_DEV)[:, None] == node_ids[None, :]).astype(
        jnp.bfloat16
    )
    columns = width // lax.axis_size("head")
    cache_part = lax.dynamic_slice_in_dim(cache, lax.axis_index("head") * columns, columns, 2)
    pulled = lax.all_to_all(
        select_rows(wanted, cache_part), "node", split_axis=0, concat_axis=0, tiled=True
    )
    prefix = select_rows(order_pick, pulled)
    prefix = lax.all_gather(prefix, "head", axis=2, tiled=True)
    q_rows = q_nope.reshape(NEW, heads_local, NOPE)
    q_pos = rotate(
        q_rope.reshape(NEW, heads_local, ROPE).astype(jnp.float32), (offset + new_index)[:, None]
    ).astype(jnp.bfloat16)
    q_pos = jnp.transpose(q_pos, (1, 0, 2))
    key_weight, value_weight = (
        lax.all_gather(w_uk, "node", axis=1, tiled=True),
        lax.all_gather(w_uv, "node", axis=1, tiled=True),
    )
    q_latent = jnp.einsum(
        "thk,hkc->htc", q_rows, key_weight, preferred_element_type=jnp.float32
    ).astype(jnp.bfloat16)
    key_rows = jnp.concatenate([prefix.reshape(hits * BLOCK, width), new_pages], axis=0)
    key_latent = key_rows[:, :LATENT]
    key_rotary = key_rows[:, LATENT:]
    prefix_seen = jnp.arange(hits * BLOCK, dtype=jnp.int32) < offset
    causal = new_index[None, :] <= new_index[:, None]
    visible = jnp.concatenate(
        [jnp.broadcast_to(prefix_seen[None, :], (NEW, hits * BLOCK)), causal], axis=1
    )
    target = max(1, 512 // NEW)
    group_size = 1
    for trial in range(1, heads_local + 1):
        if heads_local % trial == 0 and trial <= target:
            group_size = trial

    def attend(operands):
        q_part, r_part = operands
        scores = jnp.einsum("htc,kc->htk", q_part, key_latent, preferred_element_type=jnp.float32)
        scores = (
            scores
            + jnp.einsum("htr,kr->htk", r_part, key_rotary, preferred_element_type=jnp.float32)
        ) * score_scale
        scores = jnp.where(visible[None, :, :], scores, -1e30)
        row_max = jnp.max(scores, axis=-1, keepdims=True)
        expo_terms = jnp.where(visible[None, :, :], jnp.exp(scores - row_max), 0.0)
        weights = (expo_terms / jnp.sum(expo_terms, axis=-1, keepdims=True)).astype(jnp.bfloat16)
        return jnp.einsum(
            "htk,kc->htc", weights, key_latent, preferred_element_type=jnp.float32
        ).astype(jnp.bfloat16)

    groups = heads_local // group_size
    latent_out = lax.map(
        attend,
        (
            q_latent.reshape(groups, group_size, NEW, LATENT),
            q_pos.reshape(groups, group_size, NEW, ROPE),
        ),
    )
    latent_out = latent_out.reshape(heads_local, NEW, LATENT)
    projected = jnp.einsum(
        "htc,hcv->thv", latent_out, value_weight, preferred_element_type=jnp.float32
    )
    attn_out = projected.astype(jnp.bfloat16).reshape(NEW, heads_local * VHEAD)
    local_ids = jnp.arange(BLK_DEV, dtype=jnp.int32)
    new_cache = cache
    arrived = from_behind(page_blocks[0], "node", 1)
    sender = (this_node - 0 - 1 + nodes) % nodes
    slot = page_slots[sender, 0] - this_node * BLK_DEV
    new_cache = jnp.where((local_ids == slot)[:, None, None], arrived[None, :, :], new_cache)
    return (attn_out, new_cache)


def fused_kernel(
    nodes, phases, score_scale,
    pages_in, len_in, slot_in, gain_in, qn_ref, qr_ref, kv_ref, cache_ref, uk_ref, uv_ref,
    attn_ref, CB,
    UK, UV, KB, PAY, KV, Q, QR, QT, QP, QL, LAT, OUT, SEEN, pages_ref, len_ref, slot_ref, gain_ref,
    loc, e_s, e_r, c_s, c_r, n_s, n_r, q_s, q_r, t_s, t_r, m_s, m_r,
    x_s, x_r, d_s, d_r, g_s, g_r, wk_s, wk_r, wv_s, wv_r, o_s, o_r,
):
    z = lax.axis_index("node")
    y = lax.axis_index("grp")
    hd = lax.axis_index("head")
    b = z % 2
    p = z // 2
    me = 2 * y + b
    mate = z + 1 - 2 * b
    after = (z + 1) % nodes
    back = (z + nodes - 1) % nodes
    heads = UK.shape[0]
    owned = cache_ref.shape[0]
    rows_k = uk_ref.shape[1]
    rows_v = uv_ref.shape[1]
    part = BLOCK // 4
    hits = pages_ref.shape[1]
    old = nodes * BLOCK
    total = old + NEW
    near = hd + 1 - 2 * (hd % 2)
    across = (hd + 2) % 4
    team = (
        (2 * y + 1 - b, {"node": mate}),
        (2 * (1 - y) + b, {"grp": 1 - y}),
        (2 * (1 - y) + 1 - b, {"grp": 1 - y, "node": mate}),
    )
    peers = [mate]
    for j in range(1, nodes // 2):
        q = (p + j) % (nodes // 2)
        inner = jnp.where(q < p, 1, 0)
        peers = peers + [2 * q + inner, 2 * q + 1 - inner]
    outward = peers[::-1]

    def way(to):
        return (to - z + nodes) % nodes

    def road(origin):
        return (z - origin + nodes) % nodes


    barrier = pltpu.get_barrier_semaphore()
    for k in range(1, nodes):
        pl.semaphore_signal(barrier, 1, device_id={"node": (z + k) % nodes}, device_id_type=MESH)
    for to in (team[1][1], team[2][1], {"head": near}, {"head": across}):
        pl.semaphore_signal(barrier, 1, device_id=to, device_id_type=MESH)

    sends = []

    def remote(src, dst, send, recv, to):
        return pltpu.make_async_remote_copy(
            src_ref=src, dst_ref=dst, send_sem=send, recv_sem=recv, device_id=to, device_id_type=MESH
        )

    def go(*copy):
        copy = remote(*copy)
        copy.start()
        sends.append(copy)

    def arrive(block, send, recv, origin):
        remote(block, block, send, recv, origin).wait_recv()

    def rows_of(head):
        return pl.ds(pl.multiple_of(head * part, part), part)

    def cols_of(who, wide):
        return pl.ds(pl.multiple_of(who * heads * wide, 128), heads * wide)

    quarter = rows_of(hd)
    ours = pl.ds(2 * y, 2)

    def local(src, dst, slot):
        copy = pltpu.make_async_copy(src, dst, loc.at[slot])
        copy.start()
        return copy

    def mine(who):
        return pl.ds(who * heads, heads)

    early = [
        local(pages_in, pages_ref, 0),
        local(len_in, len_ref, 1),
        local(slot_in, slot_ref, 2),
        local(gain_in, gain_ref, 3),
        local(kv_ref.at[quarter, :], KV, 4),
        local(qr_ref, QR, 5),
    ]
    load = local(cache_ref, CB, 6)
    late = [
        local(qn_ref.at[:, cols_of(me, NOPE)], Q.at[me], 7),
        local(uk_ref.at[mine(me)], UK.at[:, pl.ds(pl.multiple_of(z * rows_k, rows_k), rows_k), :], 8),
        local(uv_ref.at[mine(me)], UV.at[:, pl.ds(pl.multiple_of(z * rows_v, rows_v), rows_v), :], 9),
    ]
    def weight_part(buffer, rows, first, count, node):
        return buffer.at[pl.ds(first, count), pl.ds(pl.multiple_of(node * rows, rows), rows), :]

    splits = ((0, 1), (1, heads - 1))

    def send_keys(c, to):
        first, some = splits[c]
        src = uk_ref.at[pl.ds((2 * y + to % 2) * heads + first, some)]
        k = way(to)
        go(src, weight_part(UK, rows_k, first, some, z), wk_s.at[c, k], wk_r.at[c, k], {"node": to})

    pl.semaphore_wait(barrier, nodes - 1 + 4)
    send_keys(0, outward[0])
    for copy in early:
        copy.wait()

    lane = lax.broadcasted_iota(jnp.int32, (1, 128), 1) % (ROPE // 2)
    freq = jnp.exp(lane.astype(jnp.float32) * (-2.0 * math.log(10000.0) / ROPE))

    def angles(first, count):
        at = (first + lax.broadcasted_iota(jnp.int32, (count, 128), 0)).astype(jnp.float32)
        turn = at * freq
        return jnp.cos(turn), jnp.sin(turn)

    raw = KV[...].astype(jnp.float32)
    latent = raw[:, :LATENT]
    mean = jnp.sum(latent * latent, axis=-1, keepdims=True) * (1.0 / LATENT)
    normed = latent * lax.rsqrt(mean + 1e-06) * gain_ref[...]
    rot = raw[:, LATENT:]
    swapped = jnp.concatenate([-rot[:, ROPE // 2:], rot[:, :ROPE // 2]], axis=-1)
    cosine, sine = angles(len_ref[z] + hd * part, part)
    rotary = rot * cosine[:, :ROPE] + swapped * sine[:, :ROPE]
    KB[me, nodes, quarter, :] = jnp.concatenate([normed, rotary], axis=-1).astype(jnp.bfloat16)

    column = lax.broadcasted_iota(jnp.int32, (8, old), 1)
    for i in range(2):
        session = 2 * p + i
        seen = column < 0
        for j in range(hits):
            place = column - (pages_ref[session, j] // owned) * BLOCK
            limit = jnp.minimum(len_ref[session] - j * BLOCK, BLOCK)
            seen = seen | ((place >= 0) & (place < limit))
        SEEN[2 * y + i] = jnp.where(seen, 1.0, 0.0)

    wide = 4 * heads * ROPE
    first = (lax.broadcasted_iota(jnp.int32, (NEW, wide), 1) % ROPE) < ROPE // 2
    cosine, sine = (jnp.concatenate([t] * (wide // 128), axis=1) for t in angles(len_ref[z], NEW))
    x = QR[...].astype(jnp.float32)
    ahead = pltpu.roll(x, wide - ROPE // 2, 1)
    behind = pltpu.roll(x, ROPE // 2, 1)
    QT[...] = (x * cosine + jnp.where(first, -ahead, behind) * sine).astype(jnp.bfloat16)

    load.wait()

    def local_page(session):
        found = jnp.int32(0)
        for j in range(hits):
            page = pages_ref[session, j] - z * owned
            found = jnp.where((page >= 0) & (page < owned), page, found)
        return found

    for n in range(nodes):
        PAY[n] = CB[local_page(n), quarter, :]
    for i in range(2):
        KB[2 * y + i, z, quarter, :] = CB[local_page(2 * p + i), quarter, :]

    def pages_at(group, owner):
        return KB.at[pl.ds(2 * group, 2), owner, quarter, :]

    def new_at(who):
        return KB.at[who, nodes, quarter, :]

    count = heads // phases

    def spread_part(group, origin, head):
        return KB.at[pl.ds(2 * group, 2), origin, rows_of(head), :]

    def fresh_part(head):
        return KB.at[:, nodes, rows_of(head), :]

    def spread(block, m):
        go(block, block, x_s.at[m], x_r.at[m], {"head": across})
        go(block, block, d_s.at[m], d_r.at[m], {"head": near})

    def relay(block, m):
        arrive(block, x_s.at[m], x_r.at[m], {"head": across})
        go(block, block, g_s.at[m], g_r.at[m], {"head": near})

    for to in outward:
        k = way(to)
        go(PAY.at[pl.ds((to // 2) * 2, 2)], pages_at(y, z), e_s.at[k], e_r.at[k], {"node": to})
    go(pages_at(y, z), pages_at(y, z), c_s.at[0], c_r.at[0], {"grp": 1 - y})
    spread(pages_at(y, z), 0)
    for d, (who, to) in enumerate(team):
        go(new_at(me), new_at(me), n_s.at[d], n_r.at[d], to)
    go(new_at(me), new_at(4), n_s.at[3], n_r.at[3], {"node": after})
    go(SEEN.at[ours], SEEN.at[ours], m_s.at[0], m_r.at[0], {"grp": 1 - y})
    send_keys(1, outward[0])
    for to in outward[1:]:
        send_keys(0, to)
        send_keys(1, to)

    def send_queries(d):
        who, to = team[d]
        go(QT.at[:, cols_of(who, ROPE)], QP.at[me], t_s.at[d], t_r.at[d], to)
        go(qn_ref.at[:, cols_of(who, NOPE)], Q.at[me], q_s.at[d], q_r.at[d], to)

    send_queries(0)
    QP[me] = QT[:, cols_of(me, ROPE)]
    for origin in peers:
        k = road(origin)
        block = pages_at(y, origin)
        arrive(block, e_s.at[k], e_r.at[k], {"node": origin})
        go(block, block, c_s.at[k], c_r.at[k], {"grp": 1 - y})
        spread(block, k)
    send_queries(2)
    send_queries(1)
    for f in range(phases):
        for to in outward:
            k = way(to)
            src = uv_ref.at[pl.ds((2 * y + to % 2) * heads + f * count, count)]
            go(src, weight_part(UV, rows_v, f * count, count, z), wv_s.at[f, k], wv_r.at[f, k], {"node": to})
    for origin in [z] + peers:
        k = road(origin)
        block = pages_at(1 - y, origin)
        arrive(block, c_s.at[k], c_r.at[k], {"grp": 1 - y})
        spread(block, nodes + k)
    for d, (who, to) in enumerate(team):
        arrive(new_at(who), n_s.at[d], n_r.at[d], to)
    arrive(new_at(4), n_s.at[3], n_r.at[3], {"node": back})
    spread(fresh_part(hd), 2 * nodes)
    far = near + 2 - 4 * (near // 2)
    for group in range(2):
        for origin in [z] + peers:
            relay(spread_part(y if group == 0 else 1 - y, origin, across), group * nodes + road(origin))
    relay(fresh_part(across), 2 * nodes)
    for head, r in ((near, d_r), (far, g_r)):
        for group in range(2):
            for origin in [z] + peers:
                m = group * nodes + road(origin)
                arrive(spread_part(y if group == 0 else 1 - y, origin, head), d_s.at[m], r.at[m], {"head": near})
        arrive(fresh_part(head), d_s.at[2 * nodes], r.at[2 * nodes], {"head": near})

    arrived = KB[4, nodes]
    slot = slot_ref[0, back] - z * owned

    def place(n, carry):
        CB[n] = jnp.where(slot == n, arrived, CB[n])
        return carry

    lax.fori_loop(0, owned, place, 0)

    arrive(SEEN.at[pl.ds(2 * (1 - y), 2)], m_s.at[0], m_r.at[0], {"grp": 1 - y})
    for copy in late:
        copy.wait()
    for d, (who, to) in enumerate(team):
        arrive(QP.at[who], t_s.at[d], t_r.at[d], to)
        arrive(Q.at[who], q_s.at[d], q_r.at[d], to)
    for origin in peers:
        k = road(origin)
        for c, (first_head, some) in enumerate(splits):
            block = weight_part(UK, rows_k, first_head, some, origin)
            arrive(block, wk_s.at[c, k], wk_r.at[c, k], {"node": origin})

    for h in range(heads):
        QL[h] = jnp.dot(
            Q[:, :, h * NOPE:(h + 1) * NOPE].reshape(4 * NEW, NOPE), UK[h], preferred_element_type=jnp.float32
        ).astype(jnp.bfloat16)

    contract_last = (((1,), (1,)), ((), ()))
    causal = lax.broadcasted_iota(jnp.int32, (NEW, NEW), 1) <= lax.broadcasted_iota(jnp.int32, (NEW, NEW), 0)
    causal = jnp.where(causal, 1.0, 0.0)
    for i in range(4):
        seen = jnp.concatenate([jnp.broadcast_to(SEEN[i, 0:1, :], (NEW, old)), causal], axis=1) > 0.5
        keys = KB[i].reshape(total, LATENT + ROPE)
        key_latent = keys[:, :LATENT]
        tokens = slice(i * NEW, (i + 1) * NEW)
        q_part = QL[:, tokens, :].reshape(heads * NEW, LATENT)
        r_part = jnp.concatenate([QP[i, :, h * ROPE:(h + 1) * ROPE] for h in range(heads)], axis=0)
        scores = lax.dot_general(q_part, key_latent, contract_last, preferred_element_type=jnp.float32)
        scores = scores + lax.dot_general(r_part, keys[:, LATENT:], contract_last, preferred_element_type=jnp.float32)
        scores = (scores * score_scale).reshape(heads, NEW, total)
        scores = jnp.where(seen[None], scores, -1e30)
        row_max = jnp.max(scores, axis=-1, keepdims=True)
        terms = jnp.where(seen[None], jnp.exp(scores - row_max), 0.0)
        weights = (terms / jnp.sum(terms, axis=-1, keepdims=True)).astype(jnp.bfloat16)
        mixed = jnp.dot(
            weights.reshape(heads * NEW, total), key_latent, preferred_element_type=jnp.float32
        ).astype(jnp.bfloat16)
        LAT[:, tokens, :] = mixed.reshape(heads, NEW, LATENT)

    def result_part(who, f):
        return attn_ref.at[:, pl.ds(pl.multiple_of((who * heads + f * count) * VHEAD, 128), count * VHEAD)]

    for f in range(phases):
        for origin in peers:
            k = road(origin)
            block = weight_part(UV, rows_v, f * count, count, origin)
            arrive(block, wv_s.at[f, k], wv_r.at[f, k], {"node": origin})
        for h in range(f * count, (f + 1) * count):
            OUT[:, :, h * VHEAD:(h + 1) * VHEAD] = jnp.dot(
                LAT[h], UV[h], preferred_element_type=jnp.float32
            ).astype(jnp.bfloat16).reshape(4, NEW, VHEAD)
        here = pl.ds(f * count * VHEAD, count * VHEAD)
        for d in (2, 0, 1):
            who, to = team[d]
            go(OUT.at[who, :, here], result_part(me, f), o_s.at[f, d], o_r.at[f, d], to)
    attn_ref[:, cols_of(me, VHEAD)] = OUT[me]
    for f in range(phases):
        for d, (who, to) in enumerate(team):
            arrive(result_part(who, f), o_s.at[f, d], o_r.at[f, d], to)
    for copy in sends:
        copy.wait_send()


def write_kernel(attn_ref, pages_ref, attn_out, pages_out, done):
    copies = [
        pltpu.make_async_copy(attn_ref, attn_out, done.at[0]),
        pltpu.make_async_copy(pages_ref, pages_out, done.at[1]),
    ]
    for copy in copies:
        copy.start()
    for copy in copies:
        copy.wait()


def fused_device(q_nope, q_rope, kv_new, kv_gain, cache, w_uk, w_uv, hit_pages, hit_len, page_slots):
    nodes = lax.axis_size("node")
    width = LATENT + ROPE
    heads = w_uk.shape[0] // 4
    phases = PHASES if heads % PHASES == 0 else 1
    vmem = pl.BlockSpec(memory_space=pltpu.VMEM)
    anywhere = pl.BlockSpec(memory_space=pl.ANY)
    bf16 = jnp.bfloat16
    dma = pltpu.SemaphoreType.DMA

    def pair(*shape):
        return [dma(shape), dma(shape)]

    attn, pages = pl.pallas_call(
        functools.partial(fused_kernel, nodes, phases, 1.0 / math.sqrt(NOPE + ROPE)),
        name="fused",
        out_shape=(
            pltpu.VMEM((NEW, 4 * heads * VHEAD), bf16),
            pltpu.VMEM(cache.shape, bf16),
        ),
        in_specs=[anywhere] * 10,
        out_specs=(vmem, vmem),
        scratch_shapes=[
            pltpu.VMEM((heads, NOPE, LATENT), bf16),
            pltpu.VMEM((heads, LATENT, VHEAD), bf16),
            pltpu.VMEM((5, nodes + 1, BLOCK, width), bf16),
            pltpu.VMEM((nodes, BLOCK // 4, width), bf16),
            pltpu.VMEM((BLOCK // 4, width), bf16),
            pltpu.VMEM((4, NEW, heads * NOPE), bf16),
            pltpu.VMEM((NEW, 4 * heads * ROPE), bf16),
            pltpu.VMEM((NEW, 4 * heads * ROPE), bf16),
            pltpu.VMEM((4, NEW, heads * ROPE), bf16),
            pltpu.VMEM((heads, 4 * NEW, LATENT), bf16),
            pltpu.VMEM((heads, 4 * NEW, LATENT), bf16),
            pltpu.VMEM((4, NEW, heads * VHEAD), bf16),
            pltpu.VMEM((4, 8, nodes * BLOCK), jnp.float32),
            pltpu.SMEM(hit_pages.shape, jnp.int32),
            pltpu.SMEM(hit_len.shape, jnp.int32),
            pltpu.SMEM(page_slots.shape[::-1], jnp.int32),
            pltpu.VMEM((1, LATENT), jnp.float32),
            dma((10,)),
            *pair(nodes), *pair(nodes), *pair(4), *pair(3), *pair(3), *pair(1),
            *pair(2 * nodes + 1), *pair(2 * nodes + 1), *pair(2 * nodes + 1), *pair(2, nodes), *pair(phases, nodes), *pair(phases, 3),
        ],
        compiler_params=pltpu.CompilerParams(
            collective_id=0, has_side_effects=True, vmem_limit_bytes=60 << 20
        ),
    )(hit_pages, hit_len, page_slots.T, kv_gain[None, :], q_nope, q_rope, kv_new, cache, w_uk, w_uv)
    return pl.pallas_call(
        write_kernel,
        name="write",
        out_shape=(
            jax.ShapeDtypeStruct(attn.shape, bf16),
            jax.ShapeDtypeStruct(cache.shape, bf16),
        ),
        in_specs=[vmem, vmem],
        out_specs=(anywhere, anywhere),
        scratch_shapes=[dma((2,))],
    )(*(pltpu.with_memory_space_constraint(x, pltpu.VMEM) for x in (attn, pages)))


def choose(*operands):
    w_uk, w_uv = operands[5], operands[6]
    nodes, grps, fan = (lax.axis_size(name) for name in ("node", "grp", "head"))
    fits = (
        nodes % 2 == 0
        and grps == 2
        and fan == 4
        and NEW == BLOCK
        and w_uk.shape[0] % 8 == 0
        and w_uk.shape[1] % 16 == 0
        and w_uv.shape[1] % 16 == 0
    )
    return (fused_device if fits else per_device)(*operands)


def solution(mesh):
    placed = (
        P(("grp", "node"), "head"),
        P(("grp", "node"), "head"),
        P(("grp", "node"), None),
        P(),
        P(("grp", "node"), None, None),
        P("head", "node", None),
        P("head", "node", None),
        P("grp", None),
        P("grp"),
        P("grp", None),
    )
    return jax.shard_map(
        choose,
        mesh=mesh,
        in_specs=placed,
        out_specs=(P(("grp", "node"), "head"), P(("grp", "node"), None, None)),
        check_vma=False,
    )
```

```python
import functools
import math

import jax
import jax.numpy as jnp
from jax import lax
from jax.experimental import pallas as pl
from jax.experimental.pallas import tpu as pltpu
from jax.sharding import PartitionSpec as P

LATENT = 512
ROPE = 64
NOPE = 128
VHEAD = 128
BLOCK = 64
NEW = 64
BLK_DEV = 24
PHASES = 4
MESH = pl.DeviceIdType.MESH


def from_behind(block, axis, distance):
    devices = range(lax.axis_size(axis))
    route = [((i - distance) % len(devices), i) for i in devices]
    return lax.ppermute(block, axis, route)


def rotate(values, position):
    half_rope = ROPE // 2
    inverse = 10000.0 ** (-(jnp.arange(half_rope, dtype=jnp.float32) * 2.0 / ROPE))
    angles = position.astype(jnp.float32)[..., None] * inverse
    first_half = values[..., :half_rope]
    second_half = values[..., half_rope:]
    cosine = jnp.cos(angles)
    sine = jnp.sin(angles)
    return jnp.concatenate(
        [first_half * cosine - second_half * sine, first_half * sine + second_half * cosine],
        axis=-1,
    )


def make_pages(kv_rows, kv_gain, offset):
    latent = kv_rows[:, :LATENT].astype(jnp.float32)
    normed = latent * lax.rsqrt(jnp.mean(latent * latent, axis=-1, keepdims=True) + 1e-06) * kv_gain
    rotary = rotate(
        kv_rows[:, LATENT:].astype(jnp.float32),
        offset + jnp.arange(kv_rows.shape[0], dtype=jnp.int32),
    )
    return jnp.concatenate([normed, rotary], axis=-1).astype(jnp.bfloat16)


def select_rows(selector, blocks):
    flat = blocks.reshape(blocks.shape[0], -1)
    picked = jnp.dot(selector, flat, preferred_element_type=jnp.float32).astype(jnp.bfloat16)
    return picked.reshape((selector.shape[0],) + blocks.shape[1:])


def per_device(q_nope, q_rope, kv_new, kv_gain, cache, w_uk, w_uv, hit_pages, hit_len, page_slots):
    this_node = lax.axis_index("node")
    nodes = lax.axis_size("node")
    width = LATENT + ROPE
    heads_local = w_uk.shape[0]
    hits = hit_pages.shape[1]
    pages_each = NEW // BLOCK
    score_scale = 1.0 / math.sqrt(NOPE + ROPE)
    node_ids = jnp.arange(nodes, dtype=jnp.int32)
    new_index = jnp.arange(NEW, dtype=jnp.int32)
    offset = hit_len[this_node]
    new_pages = make_pages(kv_new, kv_gain, offset)
    page_blocks = new_pages.reshape(pages_each, BLOCK, width)
    own_pages = this_node * BLK_DEV + jnp.arange(BLK_DEV, dtype=jnp.int32)
    wanted = jnp.sum(
        (hit_pages[:, :, None] == own_pages[None, None, :]).astype(jnp.int32), axis=1
    ).astype(jnp.bfloat16)
    order_pick = ((hit_pages[this_node] // BLK_DEV)[:, None] == node_ids[None, :]).astype(
        jnp.bfloat16
    )
    columns = width // lax.axis_size("head")
    cache_part = lax.dynamic_slice_in_dim(cache, lax.axis_index("head") * columns, columns, 2)
    pulled = lax.all_to_all(
        select_rows(wanted, cache_part), "node", split_axis=0, concat_axis=0, tiled=True
    )
    prefix = select_rows(order_pick, pulled)
    prefix = lax.all_gather(prefix, "head", axis=2, tiled=True)
    q_rows = q_nope.reshape(NEW, heads_local, NOPE)
    q_pos = rotate(
        q_rope.reshape(NEW, heads_local, ROPE).astype(jnp.float32), (offset + new_index)[:, None]
    ).astype(jnp.bfloat16)
    q_pos = jnp.transpose(q_pos, (1, 0, 2))
    key_weight, value_weight = (
        lax.all_gather(w_uk, "node", axis=1, tiled=True),
        lax.all_gather(w_uv, "node", axis=1, tiled=True),
    )
    q_latent = jnp.einsum(
        "thk,hkc->htc", q_rows, key_weight, preferred_element_type=jnp.float32
    ).astype(jnp.bfloat16)
    key_rows = jnp.concatenate([prefix.reshape(hits * BLOCK, width), new_pages], axis=0)
    key_latent = key_rows[:, :LATENT]
    key_rotary = key_rows[:, LATENT:]
    prefix_seen = jnp.arange(hits * BLOCK, dtype=jnp.int32) < offset
    causal = new_index[None, :] <= new_index[:, None]
    visible = jnp.concatenate(
        [jnp.broadcast_to(prefix_seen[None, :], (NEW, hits * BLOCK)), causal], axis=1
    )
    target = max(1, 512 // NEW)
    group_size = 1
    for trial in range(1, heads_local + 1):
        if heads_local % trial == 0 and trial <= target:
            group_size = trial

    def attend(operands):
        q_part, r_part = operands
        scores = jnp.einsum("htc,kc->htk", q_part, key_latent, preferred_element_type=jnp.float32)
        scores = (
            scores
            + jnp.einsum("htr,kr->htk", r_part, key_rotary, preferred_element_type=jnp.float32)
        ) * score_scale
        scores = jnp.where(visible[None, :, :], scores, -1e30)
        row_max = jnp.max(scores, axis=-1, keepdims=True)
        expo_terms = jnp.where(visible[None, :, :], jnp.exp(scores - row_max), 0.0)
        weights = (expo_terms / jnp.sum(expo_terms, axis=-1, keepdims=True)).astype(jnp.bfloat16)
        return jnp.einsum(
            "htk,kc->htc", weights, key_latent, preferred_element_type=jnp.float32
        ).astype(jnp.bfloat16)

    groups = heads_local // group_size
    latent_out = lax.map(
        attend,
        (
            q_latent.reshape(groups, group_size, NEW, LATENT),
            q_pos.reshape(groups, group_size, NEW, ROPE),
        ),
    )
    latent_out = latent_out.reshape(heads_local, NEW, LATENT)
    projected = jnp.einsum(
        "htc,hcv->thv", latent_out, value_weight, preferred_element_type=jnp.float32
    )
    attn_out = projected.astype(jnp.bfloat16).reshape(NEW, heads_local * VHEAD)
    local_ids = jnp.arange(BLK_DEV, dtype=jnp.int32)
    new_cache = cache
    arrived = from_behind(page_blocks[0], "node", 1)
    sender = (this_node - 0 - 1 + nodes) % nodes
    slot = page_slots[sender, 0] - this_node * BLK_DEV
    new_cache = jnp.where((local_ids == slot)[:, None, None], arrived[None, :, :], new_cache)
    return (attn_out, new_cache)


def fused_kernel(
    nodes, phases, score_scale,
    pages_in, len_in, slot_in, gain_in, qn_ref, qr_ref, kv_ref, cache_ref, uk_ref, uv_ref,
    attn_ref, CB,
    UK, UV, KB, PAY, KV, Q, QR, QT, QP, QL, LAT, OUT, SEEN, pages_ref, len_ref, slot_ref, gain_ref,
    loc, e_s, e_r, c_s, c_r, n_s, n_r, q_s, q_r, t_s, t_r, m_s, m_r,
    x_s, x_r, d_s, d_r, g_s, g_r, wk_s, wk_r, wv_s, wv_r, fk_s, fv_s, o_s, o_r, ready,
):
    z = lax.axis_index("node")
    y = lax.axis_index("grp")
    hd = lax.axis_index("head")
    b = z % 2
    p = z // 2
    me = 2 * y + b
    mate = z + 1 - 2 * b
    after = (z + 1) % nodes
    back = (z + nodes - 1) % nodes
    heads = UK.shape[0]
    owned = cache_ref.shape[0]
    rows_k = uk_ref.shape[1]
    rows_v = uv_ref.shape[1]
    part = BLOCK // 4
    hits = pages_ref.shape[1]
    old = nodes * BLOCK
    total = old + NEW
    near = hd + 1 - 2 * (hd % 2)
    across = (hd + 2) % 4
    team = (
        (2 * y + 1 - b, {"node": mate}),
        (2 * (1 - y) + b, {"grp": 1 - y}),
        (2 * (1 - y) + 1 - b, {"grp": 1 - y, "node": mate}),
    )
    inside, outside = 2 - p, 3 - 3 * p
    inner = b + p == 1
    outer = b + p != 1
    peers = (mate, inside, outside)

    def way(to):
        return (to - z + nodes) % nodes

    def road(origin):
        return (z - origin + nodes) % nodes

    barrier = pltpu.get_barrier_semaphore()
    others = (
        (y == 0, nodes, team[1][1]),
        (y == 0, nodes + 1, team[2][1]),
        (hd % 2 == 0, nodes + 2, {"head": near}),
        (hd < 2, nodes + 3, {"head": across}),
    )

    def tell(semaphore, condition, to):
        @pl.when(condition)
        def _():
            pl.semaphore_signal(semaphore, 1, device_id=to, device_id_type=MESH)

    for k in range(1, nodes):
        tell(barrier, z + k < nodes, {"node": (z + k) % nodes})
    for first_in, at, to in others:
        tell(barrier, first_in, to)

    sends = []
    relayed = []

    def remote(src, dst, send, recv, to):
        return pltpu.make_async_remote_copy(
            src_ref=src, dst_ref=dst, send_sem=send, recv_sem=recv, device_id=to, device_id_type=MESH
        )

    def go(*copy):
        copy = remote(*copy)
        copy.start()
        sends.append(copy)

    def arrive(block, send, recv, origin):
        remote(block, block, send, recv, origin).wait_recv()

    def rows_of(head):
        return pl.ds(pl.multiple_of(head * part, part), part)

    def cols_of(who, wide):
        return pl.ds(pl.multiple_of(who * heads * wide, 128), heads * wide)

    quarter = rows_of(hd)
    ours = pl.ds(2 * y, 2)

    def local(src, dst, slot):
        copy = pltpu.make_async_copy(src, dst, loc.at[slot])
        copy.start()
        return copy

    def mine(who):
        return pl.ds(who * heads, heads)

    early = [
        local(pages_in, pages_ref, 0),
        local(len_in, len_ref, 1),
        local(slot_in, slot_ref, 2),
        local(gain_in, gain_ref, 3),
        local(kv_ref.at[quarter, :], KV, 4),
        local(qr_ref, QR, 5),
    ]
    load = local(cache_ref, CB, 6)
    late = [
        local(qn_ref.at[:, cols_of(me, NOPE)], Q.at[me], 7),
        local(uk_ref.at[mine(me)], UK.at[:, pl.ds(pl.multiple_of(z * rows_k, rows_k), rows_k), :], 8),
        local(uv_ref.at[mine(me)], UV.at[:, pl.ds(pl.multiple_of(z * rows_v, rows_v), rows_v), :], 9),
    ]
    def weight_part(buffer, rows, first, count, node):
        return buffer.at[pl.ds(first, count), pl.ds(pl.multiple_of(node * rows, rows), rows), :]

    splits = ((0, 2), (2, heads - 2))

    def key_copy(c, to):
        first, some = splits[c]
        src = uk_ref.at[pl.ds((2 * y + to % 2) * heads + first, some)]
        k = way(to)
        return remote(src, weight_part(UK, rows_k, first, some, z), wk_s.at[c, k], wk_r.at[c, k], {"node": to})

    def send_keys(c, to):
        copy = key_copy(c, to)
        copy.start()
        sends.append(copy)

    known = z + 2 * y + hd % 2 + hd // 2

    @pl.when(known > 0)
    def _():
        pl.semaphore_wait(barrier, known)

    for k in range(1, nodes):
        tell(ready.at[k], z >= k, {"node": (z + nodes - k) % nodes})
    for first_in, at, to in others:
        tell(ready.at[at], jnp.logical_not(first_in), to)

    def meet(condition, at):
        @pl.when(condition)
        def _():
            pl.semaphore_wait(ready.at[at], 1)

    def meet_node(to):
        meet(to > z, way(to))

    def meet_other(i):
        meet(others[i][0], others[i][1])

    opening = key_copy(0, inside)
    sends.append(opening)
    pl.when(inside < z)(opening.start)

    for copy in early:
        copy.wait()

    lane = lax.broadcasted_iota(jnp.int32, (1, 128), 1) % (ROPE // 2)
    freq = jnp.exp(lane.astype(jnp.float32) * (-2.0 * math.log(10000.0) / ROPE))

    def angles(first, count):
        at = (first + lax.broadcasted_iota(jnp.int32, (count, 128), 0)).astype(jnp.float32)
        turn = at * freq
        return jnp.cos(turn), jnp.sin(turn)

    raw = KV[...].astype(jnp.float32)
    latent = raw[:, :LATENT]
    mean = jnp.sum(latent * latent, axis=-1, keepdims=True) * (1.0 / LATENT)
    normed = latent * lax.rsqrt(mean + 1e-06) * gain_ref[...]
    rot = raw[:, LATENT:]
    swapped = jnp.concatenate([-rot[:, ROPE // 2:], rot[:, :ROPE // 2]], axis=-1)
    cosine, sine = angles(len_ref[z] + hd * part, part)
    rotary = rot * cosine[:, :ROPE] + swapped * sine[:, :ROPE]
    KB[me, nodes, quarter, :] = jnp.concatenate([normed, rotary], axis=-1).astype(jnp.bfloat16)

    column = lax.broadcasted_iota(jnp.int32, (8, old), 1)
    for i in range(2):
        session = 2 * p + i
        seen = column < 0
        for j in range(hits):
            place = column - (pages_ref[session, j] // owned) * BLOCK
            limit = jnp.minimum(len_ref[session] - j * BLOCK, BLOCK)
            seen = seen | ((place >= 0) & (place < limit))
        SEEN[2 * y + i] = jnp.where(seen, 1.0, 0.0)

    wide = 4 * heads * ROPE
    first = (lax.broadcasted_iota(jnp.int32, (NEW, wide), 1) % ROPE) < ROPE // 2
    cosine, sine = (jnp.concatenate([t] * (wide // 128), axis=1) for t in angles(len_ref[z], NEW))
    x = QR[...].astype(jnp.float32)
    ahead = pltpu.roll(x, wide - ROPE // 2, 1)
    behind = pltpu.roll(x, ROPE // 2, 1)
    QT[...] = (x * cosine + jnp.where(first, -ahead, behind) * sine).astype(jnp.bfloat16)

    load.wait()

    def local_page(session):
        found = jnp.int32(0)
        for j in range(hits):
            page = pages_ref[session, j] - z * owned
            found = jnp.where((page >= 0) & (page < owned), page, found)
        return found

    for n in range(nodes):
        PAY[n] = CB[local_page(n), quarter, :]
    for i in range(2):
        KB[2 * y + i, z, quarter, :] = CB[local_page(2 * p + i), quarter, :]

    def pages_at(group, owner):
        return KB.at[pl.ds(2 * group, 2), owner, quarter, :]

    def new_at(who):
        return KB.at[who, nodes, quarter, :]

    count = heads // phases

    def spread_part(group, origin, head):
        return KB.at[pl.ds(2 * group, 2), origin, rows_of(head), :]

    def fresh_part(head):
        return KB.at[:, nodes, rows_of(head), :]

    def spread(block, m):
        go(block, block, x_s.at[m], x_r.at[m], {"head": across})
        go(block, block, d_s.at[m], d_r.at[m], {"head": near})

    def relay(block, m):
        arrive(block, x_s.at[m], x_r.at[m], {"head": across})
        go(block, block, g_s.at[m], g_r.at[m], {"head": near})

    def send_queries(d):
        who, to = team[d]
        go(QT.at[:, cols_of(who, ROPE)], QP.at[me], t_s.at[d], t_r.at[d], to)
        go(qn_ref.at[:, cols_of(who, NOPE)], Q.at[me], q_s.at[d], q_r.at[d], to)

    def page_copy(to):
        k = way(to)
        return remote(PAY.at[pl.ds((to // 2) * 2, 2)], pages_at(y, z), e_s.at[k], e_r.at[k], {"node": to})

    def send_new(d):
        go(new_at(me), new_at(me), n_s.at[d], n_r.at[d], team[d][1])

    copies = [page_copy(to) for to in peers]
    sends.extend(copies)
    pl.when(outside < z)(copies[2].start)
    meet_node(inside)
    copies[1].start()
    meet_node(mate)
    copies[0].start()
    send_new(0)
    pl.when(inside > z)(opening.start)
    meet_other(0)
    go(pages_at(y, z), pages_at(y, z), c_s.at[0], c_r.at[0], {"grp": 1 - y})
    send_new(1)
    go(SEEN.at[ours], SEEN.at[ours], m_s.at[0], m_r.at[0], {"grp": 1 - y})
    meet_other(1)
    send_new(2)
    def go_when(condition, copy):
        pl.when(condition)(copy.start)
        relayed.append((condition, copy))

    def key_block(c, node):
        return weight_part(UK, rows_k, *splits[c], node)

    def value_block(f, node):
        return weight_part(UV, rows_v, f * count, count, node)

    def value_copy(f, to):
        k = way(to)
        src = uv_ref.at[pl.ds((2 * y + to % 2) * heads + f * count, count)]
        return remote(src, value_block(f, z), wv_s.at[f, k], wv_r.at[f, k], {"node": to})

    def send_values(f, to):
        copy = value_copy(f, to)
        copy.start()
        sends.append(copy)

    send_keys(1, inside)
    send_keys(0, mate)
    send_keys(1, mate)
    meet_other(2)
    meet_other(3)
    spread(pages_at(y, z), 0)
    meet_node(outside)
    pl.when(outside > z)(copies[2].start)
    go(new_at(me), new_at(4), n_s.at[3], n_r.at[3], {"node": after})
    send_queries(0)
    send_queries(2)
    for c in range(2):
        go_when(inner, key_copy(c, outside))

    QP[me] = QT[:, cols_of(me, ROPE)]
    for origin in peers:
        k = road(origin)
        block = pages_at(y, origin)
        arrive(block, e_s.at[k], e_r.at[k], {"node": origin})
        go(block, block, c_s.at[k], c_r.at[k], {"grp": 1 - y})
        spread(block, k)
    send_queries(1)
    mated, hop = road(mate), (outside - mate + nodes) % nodes

    def arrive_keys(c, origin):
        k = road(origin)
        block = key_block(c, origin)
        arrive(block, wk_s.at[c, k], wk_r.at[c, k], {"node": origin})

    def arrive_values(f, origin):
        k = road(origin)
        block = value_block(f, origin)
        arrive(block, wv_s.at[f, k], wv_r.at[f, k], {"node": origin})

    for c in range(2):
        pl.when(inner)(functools.partial(arrive_keys, c, mate))
        block = key_block(c, mate)
        go_when(inner, remote(block, block, fk_s.at[c], wk_r.at[c, hop], {"node": outside}))
    send_values(0, mate)
    send_values(1, mate)
    send_values(2, mate)
    send_values(3, mate)
    go_when(inner, value_copy(0, outside))
    send_values(0, inside)
    go_when(inner, value_copy(1, outside))
    send_values(1, inside)
    for origin in (z, *peers):
        k = road(origin)
        block = pages_at(1 - y, origin)
        arrive(block, c_s.at[k], c_r.at[k], {"grp": 1 - y})
        spread(block, nodes + k)
    for d, (who, to) in enumerate(team):
        arrive(new_at(who), n_s.at[d], n_r.at[d], to)
    arrive(new_at(4), n_s.at[3], n_r.at[3], {"node": back})
    spread(fresh_part(hd), 2 * nodes)
    far = near + 2 - 4 * (near // 2)
    for group in range(2):
        for origin in (z, *peers):
            relay(spread_part(y if group == 0 else 1 - y, origin, across), group * nodes + road(origin))
    relay(fresh_part(across), 2 * nodes)
    for head, r in ((near, d_r), (far, g_r)):
        for group in range(2):
            for origin in (z, *peers):
                m = group * nodes + road(origin)
                arrive(spread_part(y if group == 0 else 1 - y, origin, head), d_s.at[m], r.at[m], {"head": near})
        arrive(fresh_part(head), d_s.at[2 * nodes], r.at[2 * nodes], {"head": near})

    arrived = KB[4, nodes]
    slot = slot_ref[0, back] - z * owned

    def place(n, carry):
        CB[n] = jnp.where(slot == n, arrived, CB[n])
        return carry

    lax.fori_loop(0, owned, place, 0)

    arrive(SEEN.at[pl.ds(2 * (1 - y), 2)], m_s.at[0], m_r.at[0], {"grp": 1 - y})
    for copy in late:
        copy.wait()
    for d, (who, to) in enumerate(team):
        arrive(QP.at[who], t_s.at[d], t_r.at[d], to)
        arrive(Q.at[who], q_s.at[d], q_r.at[d], to)
    for f in (0, 1):
        pl.when(inner)(functools.partial(arrive_values, f, mate))
        block = value_block(f, mate)
        go_when(inner, remote(block, block, fv_s.at[f], wv_r.at[f, hop], {"node": outside}))
    go_when(inner, value_copy(2, outside))
    send_values(2, inside)
    go_when(inner, value_copy(3, outside))
    send_values(3, inside)
    for f in (2, 3):
        pl.when(inner)(functools.partial(arrive_values, f, mate))
        block = value_block(f, mate)
        go_when(inner, remote(block, block, fv_s.at[f], wv_r.at[f, hop], {"node": outside}))
    for c in range(2):
        pl.when(outer)(functools.partial(arrive_keys, c, mate))
        for origin in (inside, outside):
            arrive_keys(c, origin)

    for h in range(heads):
        QL[h] = jnp.dot(
            Q[:, :, h * NOPE:(h + 1) * NOPE].reshape(4 * NEW, NOPE), UK[h], preferred_element_type=jnp.float32
        ).astype(jnp.bfloat16)

    contract_last = (((1,), (1,)), ((), ()))
    causal = lax.broadcasted_iota(jnp.int32, (NEW, NEW), 1) <= lax.broadcasted_iota(jnp.int32, (NEW, NEW), 0)
    causal = jnp.where(causal, 1.0, 0.0)
    for i in range(4):
        seen = jnp.concatenate([jnp.broadcast_to(SEEN[i, 0:1, :], (NEW, old)), causal], axis=1) > 0.5
        keys = KB[i].reshape(total, LATENT + ROPE)
        key_latent = keys[:, :LATENT]
        tokens = slice(i * NEW, (i + 1) * NEW)
        q_part = QL[:, tokens, :].reshape(heads * NEW, LATENT)
        r_part = jnp.concatenate([QP[i, :, h * ROPE:(h + 1) * ROPE] for h in range(heads)], axis=0)
        scores = lax.dot_general(q_part, key_latent, contract_last, preferred_element_type=jnp.float32)
        scores = scores + lax.dot_general(r_part, keys[:, LATENT:], contract_last, preferred_element_type=jnp.float32)
        scores = (scores * score_scale).reshape(heads, NEW, total)
        scores = jnp.where(seen[None], scores, -1e30)
        row_max = jnp.max(scores, axis=-1, keepdims=True)
        terms = jnp.where(seen[None], jnp.exp(scores - row_max), 0.0)
        weights = (terms / jnp.sum(terms, axis=-1, keepdims=True)).astype(jnp.bfloat16)
        mixed = jnp.dot(
            weights.reshape(heads * NEW, total), key_latent, preferred_element_type=jnp.float32
        ).astype(jnp.bfloat16)
        LAT[:, tokens, :] = mixed.reshape(heads, NEW, LATENT)

    def result_part(who, f):
        return attn_ref.at[:, pl.ds(pl.multiple_of((who * heads + f * count) * VHEAD, 128), count * VHEAD)]

    for f in range(phases):
        pl.when(outer)(functools.partial(arrive_values, f, mate))
        for origin in (inside, outside):
            arrive_values(f, origin)
        for h in range(f * count, (f + 1) * count):
            OUT[:, :, h * VHEAD:(h + 1) * VHEAD] = jnp.dot(
                LAT[h], UV[h], preferred_element_type=jnp.float32
            ).astype(jnp.bfloat16).reshape(4, NEW, VHEAD)
        here = pl.ds(f * count * VHEAD, count * VHEAD)
        for d in (2, 0, 1):
            who, to = team[d]
            go(OUT.at[who, :, here], result_part(me, f), o_s.at[f, d], o_r.at[f, d], to)
    attn_ref[:, cols_of(me, VHEAD)] = OUT[me]
    for f in range(phases):
        for d, (who, to) in enumerate(team):
            arrive(result_part(who, f), o_s.at[f, d], o_r.at[f, d], to)
    for copy in sends:
        copy.wait_send()
    for condition, copy in relayed:
        pl.when(condition)(copy.wait_send)


def write_kernel(attn_ref, pages_ref, attn_out, pages_out, done):
    copies = [
        pltpu.make_async_copy(attn_ref, attn_out, done.at[0]),
        pltpu.make_async_copy(pages_ref, pages_out, done.at[1]),
    ]
    for copy in copies:
        copy.start()
    for copy in copies:
        copy.wait()


def fused_device(q_nope, q_rope, kv_new, kv_gain, cache, w_uk, w_uv, hit_pages, hit_len, page_slots):
    nodes = lax.axis_size("node")
    width = LATENT + ROPE
    heads = w_uk.shape[0] // 4
    phases = PHASES if heads % PHASES == 0 else 1
    vmem = pl.BlockSpec(memory_space=pltpu.VMEM)
    anywhere = pl.BlockSpec(memory_space=pl.ANY)
    bf16 = jnp.bfloat16
    dma = pltpu.SemaphoreType.DMA

    def pair(*shape):
        return [dma(shape), dma(shape)]

    attn, pages = pl.pallas_call(
        functools.partial(fused_kernel, nodes, phases, 1.0 / math.sqrt(NOPE + ROPE)),
        name="fused",
        out_shape=(
            pltpu.VMEM((NEW, 4 * heads * VHEAD), bf16),
            pltpu.VMEM(cache.shape, bf16),
        ),
        in_specs=[anywhere] * 10,
        out_specs=(vmem, vmem),
        scratch_shapes=[
            pltpu.VMEM((heads, NOPE, LATENT), bf16),
            pltpu.VMEM((heads, LATENT, VHEAD), bf16),
            pltpu.VMEM((5, nodes + 1, BLOCK, width), bf16),
            pltpu.VMEM((nodes, BLOCK // 4, width), bf16),
            pltpu.VMEM((BLOCK // 4, width), bf16),
            pltpu.VMEM((4, NEW, heads * NOPE), bf16),
            pltpu.VMEM((NEW, 4 * heads * ROPE), bf16),
            pltpu.VMEM((NEW, 4 * heads * ROPE), bf16),
            pltpu.VMEM((4, NEW, heads * ROPE), bf16),
            pltpu.VMEM((heads, 4 * NEW, LATENT), bf16),
            pltpu.VMEM((heads, 4 * NEW, LATENT), bf16),
            pltpu.VMEM((4, NEW, heads * VHEAD), bf16),
            pltpu.VMEM((4, 8, nodes * BLOCK), jnp.float32),
            pltpu.SMEM(hit_pages.shape, jnp.int32),
            pltpu.SMEM(hit_len.shape, jnp.int32),
            pltpu.SMEM(page_slots.shape[::-1], jnp.int32),
            pltpu.VMEM((1, LATENT), jnp.float32),
            dma((10,)),
            *pair(nodes), *pair(nodes), *pair(4), *pair(3), *pair(3), *pair(1),
            *pair(2 * nodes + 1), *pair(2 * nodes + 1), *pair(2 * nodes + 1), *pair(2, nodes), *pair(phases, nodes), dma((2,)), dma((phases,)), *pair(phases, 3),
            pltpu.SemaphoreType.REGULAR((nodes + 4,)),
        ],
        compiler_params=pltpu.CompilerParams(
            collective_id=0, has_side_effects=True, vmem_limit_bytes=60 << 20
        ),
    )(hit_pages, hit_len, page_slots.T, kv_gain[None, :], q_nope, q_rope, kv_new, cache, w_uk, w_uv)
    return pl.pallas_call(
        write_kernel,
        name="write",
        out_shape=(
            jax.ShapeDtypeStruct(attn.shape, bf16),
            jax.ShapeDtypeStruct(cache.shape, bf16),
        ),
        in_specs=[vmem, vmem],
        out_specs=(anywhere, anywhere),
        scratch_shapes=[dma((2,))],
    )(*(pltpu.with_memory_space_constraint(x, pltpu.VMEM) for x in (attn, pages)))


def choose(*operands):
    w_uk, w_uv = operands[5], operands[6]
    nodes, grps, fan = (lax.axis_size(name) for name in ("node", "grp", "head"))
    fits = (
        (nodes, grps, fan) == (4, 2, 4)
        and NEW == BLOCK
        and w_uk.shape[0] % 8 == 0
        and w_uk.shape[1] % 16 == 0
        and w_uv.shape[1] % 16 == 0
    )
    return (fused_device if fits else per_device)(*operands)


def solution(mesh):
    placed = (
        P(("grp", "node"), "head"),
        P(("grp", "node"), "head"),
        P(("grp", "node"), None),
        P(),
        P(("grp", "node"), None, None),
        P("head", "node", None),
        P("head", "node", None),
        P("grp", None),
        P("grp"),
        P("grp", None),
    )
    return jax.shard_map(
        choose,
        mesh=mesh,
        in_specs=placed,
        out_specs=(P(("grp", "node"), "head"), P(("grp", "node"), None, None)),
        check_vma=False,
    )
```

```python
import functools
import math

import jax
import jax.numpy as jnp
from jax import lax
from jax.experimental import pallas as pl
from jax.experimental.pallas import tpu as pltpu
from jax.sharding import PartitionSpec as P

LATENT = 512
ROPE = 64
NOPE = 128
VHEAD = 128
BLOCK = 64
NEW = 64
BLK_DEV = 24
PHASES = 4
MESH = pl.DeviceIdType.MESH


def from_behind(block, axis, distance):
    devices = range(lax.axis_size(axis))
    route = [((i - distance) % len(devices), i) for i in devices]
    return lax.ppermute(block, axis, route)


def rotate(values, position):
    half_rope = ROPE // 2
    inverse = 10000.0 ** (-(jnp.arange(half_rope, dtype=jnp.float32) * 2.0 / ROPE))
    angles = position.astype(jnp.float32)[..., None] * inverse
    first_half = values[..., :half_rope]
    second_half = values[..., half_rope:]
    cosine = jnp.cos(angles)
    sine = jnp.sin(angles)
    return jnp.concatenate(
        [first_half * cosine - second_half * sine, first_half * sine + second_half * cosine],
        axis=-1,
    )


def make_pages(kv_rows, kv_gain, offset):
    latent = kv_rows[:, :LATENT].astype(jnp.float32)
    normed = latent * lax.rsqrt(jnp.mean(latent * latent, axis=-1, keepdims=True) + 1e-06) * kv_gain
    rotary = rotate(
        kv_rows[:, LATENT:].astype(jnp.float32),
        offset + jnp.arange(kv_rows.shape[0], dtype=jnp.int32),
    )
    return jnp.concatenate([normed, rotary], axis=-1).astype(jnp.bfloat16)


def select_rows(selector, blocks):
    flat = blocks.reshape(blocks.shape[0], -1)
    picked = jnp.dot(selector, flat, preferred_element_type=jnp.float32).astype(jnp.bfloat16)
    return picked.reshape((selector.shape[0],) + blocks.shape[1:])


def per_device(q_nope, q_rope, kv_new, kv_gain, cache, w_uk, w_uv, hit_pages, hit_len, page_slots):
    this_node = lax.axis_index("node")
    nodes = lax.axis_size("node")
    width = LATENT + ROPE
    heads_local = w_uk.shape[0]
    hits = hit_pages.shape[1]
    pages_each = NEW // BLOCK
    score_scale = 1.0 / math.sqrt(NOPE + ROPE)
    node_ids = jnp.arange(nodes, dtype=jnp.int32)
    new_index = jnp.arange(NEW, dtype=jnp.int32)
    offset = hit_len[this_node]
    new_pages = make_pages(kv_new, kv_gain, offset)
    page_blocks = new_pages.reshape(pages_each, BLOCK, width)
    own_pages = this_node * BLK_DEV + jnp.arange(BLK_DEV, dtype=jnp.int32)
    wanted = jnp.sum(
        (hit_pages[:, :, None] == own_pages[None, None, :]).astype(jnp.int32), axis=1
    ).astype(jnp.bfloat16)
    order_pick = ((hit_pages[this_node] // BLK_DEV)[:, None] == node_ids[None, :]).astype(
        jnp.bfloat16
    )
    columns = width // lax.axis_size("head")
    cache_part = lax.dynamic_slice_in_dim(cache, lax.axis_index("head") * columns, columns, 2)
    pulled = lax.all_to_all(
        select_rows(wanted, cache_part), "node", split_axis=0, concat_axis=0, tiled=True
    )
    prefix = select_rows(order_pick, pulled)
    prefix = lax.all_gather(prefix, "head", axis=2, tiled=True)
    q_rows = q_nope.reshape(NEW, heads_local, NOPE)
    q_pos = rotate(
        q_rope.reshape(NEW, heads_local, ROPE).astype(jnp.float32), (offset + new_index)[:, None]
    ).astype(jnp.bfloat16)
    q_pos = jnp.transpose(q_pos, (1, 0, 2))
    key_weight, value_weight = (
        lax.all_gather(w_uk, "node", axis=1, tiled=True),
        lax.all_gather(w_uv, "node", axis=1, tiled=True),
    )
    q_latent = jnp.einsum(
        "thk,hkc->htc", q_rows, key_weight, preferred_element_type=jnp.float32
    ).astype(jnp.bfloat16)
    key_rows = jnp.concatenate([prefix.reshape(hits * BLOCK, width), new_pages], axis=0)
    key_latent = key_rows[:, :LATENT]
    key_rotary = key_rows[:, LATENT:]
    prefix_seen = jnp.arange(hits * BLOCK, dtype=jnp.int32) < offset
    causal = new_index[None, :] <= new_index[:, None]
    visible = jnp.concatenate(
        [jnp.broadcast_to(prefix_seen[None, :], (NEW, hits * BLOCK)), causal], axis=1
    )
    target = max(1, 512 // NEW)
    group_size = 1
    for trial in range(1, heads_local + 1):
        if heads_local % trial == 0 and trial <= target:
            group_size = trial

    def attend(operands):
        q_part, r_part = operands
        scores = jnp.einsum("htc,kc->htk", q_part, key_latent, preferred_element_type=jnp.float32)
        scores = (
            scores
            + jnp.einsum("htr,kr->htk", r_part, key_rotary, preferred_element_type=jnp.float32)
        ) * score_scale
        scores = jnp.where(visible[None, :, :], scores, -1e30)
        row_max = jnp.max(scores, axis=-1, keepdims=True)
        expo_terms = jnp.where(visible[None, :, :], jnp.exp(scores - row_max), 0.0)
        weights = (expo_terms / jnp.sum(expo_terms, axis=-1, keepdims=True)).astype(jnp.bfloat16)
        return jnp.einsum(
            "htk,kc->htc", weights, key_latent, preferred_element_type=jnp.float32
        ).astype(jnp.bfloat16)

    groups = heads_local // group_size
    latent_out = lax.map(
        attend,
        (
            q_latent.reshape(groups, group_size, NEW, LATENT),
            q_pos.reshape(groups, group_size, NEW, ROPE),
        ),
    )
    latent_out = latent_out.reshape(heads_local, NEW, LATENT)
    projected = jnp.einsum(
        "htc,hcv->thv", latent_out, value_weight, preferred_element_type=jnp.float32
    )
    attn_out = projected.astype(jnp.bfloat16).reshape(NEW, heads_local * VHEAD)
    local_ids = jnp.arange(BLK_DEV, dtype=jnp.int32)
    new_cache = cache
    arrived = from_behind(page_blocks[0], "node", 1)
    sender = (this_node - 0 - 1 + nodes) % nodes
    slot = page_slots[sender, 0] - this_node * BLK_DEV
    new_cache = jnp.where((local_ids == slot)[:, None, None], arrived[None, :, :], new_cache)
    return (attn_out, new_cache)


def fused_kernel(
    nodes, phases, score_scale,
    pages_in, len_in, slot_in, gain_in, qn_ref, qr_ref, kv_ref, cache_ref, uk_ref, uv_ref,
    attn_ref, CB,
    UK, UV, KB, PAY, KV, Q, QR, QT, QP, QL, LAT, OUT, SEEN, pages_ref, len_ref, slot_ref, gain_ref,
    loc, e_s, e_r, c_s, c_r, n_s, n_r, q_s, q_r, t_s, t_r, m_s, m_r,
    x_s, x_r, d_s, d_r, g_s, g_r, wk_s, wk_r, wv_s, wv_r, fk_s, fv_s, o_s, o_r, ready,
):
    z = lax.axis_index("node")
    y = lax.axis_index("grp")
    hd = lax.axis_index("head")
    b = z % 2
    p = z // 2
    me = 2 * y + b
    mate = z + 1 - 2 * b
    after = (z + 1) % nodes
    back = (z + nodes - 1) % nodes
    heads = UK.shape[0]
    owned = cache_ref.shape[0]
    rows_k = uk_ref.shape[1]
    rows_v = uv_ref.shape[1]
    part = BLOCK // 4
    hits = pages_ref.shape[1]
    old = nodes * BLOCK
    total = old + NEW
    near = hd + 1 - 2 * (hd % 2)
    across = (hd + 2) % 4
    team = (
        (2 * y + 1 - b, {"node": mate}),
        (2 * (1 - y) + b, {"grp": 1 - y}),
        (2 * (1 - y) + 1 - b, {"grp": 1 - y, "node": mate}),
    )
    inside, outside = 2 - p, 3 - 3 * p
    inner = b + p == 1
    outer = b + p != 1
    peers = (mate, inside, outside)

    def way(to):
        return (to - z + nodes) % nodes

    def road(origin):
        return (z - origin + nodes) % nodes

    barrier = pltpu.get_barrier_semaphore()
    others = (
        (y == 0, nodes, team[1][1]),
        (y == 0, nodes + 1, team[2][1]),
        (hd % 2 == 0, nodes + 2, {"head": near}),
        (hd < 2, nodes + 3, {"head": across}),
    )

    def tell(semaphore, condition, to):
        @pl.when(condition)
        def _():
            pl.semaphore_signal(semaphore, 1, device_id=to, device_id_type=MESH)

    for k in range(1, nodes):
        tell(barrier, z + k < nodes, {"node": (z + k) % nodes})
    for first_in, at, to in others:
        tell(barrier, first_in, to)

    sends = []
    relayed = []

    def remote(src, dst, send, recv, to):
        return pltpu.make_async_remote_copy(
            src_ref=src, dst_ref=dst, send_sem=send, recv_sem=recv, device_id=to, device_id_type=MESH
        )

    def go(*copy):
        copy = remote(*copy)
        copy.start()
        sends.append(copy)

    def arrive(block, send, recv, origin):
        remote(block, block, send, recv, origin).wait_recv()

    def rows_of(head):
        return pl.ds(pl.multiple_of(head * part, part), part)

    def cols_of(who, wide):
        return pl.ds(pl.multiple_of(who * heads * wide, 128), heads * wide)

    quarter = rows_of(hd)
    ours = pl.ds(2 * y, 2)

    def local(src, dst, slot):
        copy = pltpu.make_async_copy(src, dst, loc.at[slot])
        copy.start()
        return copy

    def mine(who):
        return pl.ds(who * heads, heads)

    early = [
        local(pages_in, pages_ref, 0),
        local(len_in, len_ref, 1),
        local(slot_in, slot_ref, 2),
        local(gain_in, gain_ref, 3),
        local(kv_ref.at[quarter, :], KV, 4),
        local(qr_ref, QR, 5),
    ]
    load = local(cache_ref, CB, 6)
    late = [
        local(qn_ref.at[:, cols_of(me, NOPE)], Q.at[me], 7),
        local(uk_ref.at[mine(me)], UK.at[:, pl.ds(pl.multiple_of(z * rows_k, rows_k), rows_k), :], 8),
        local(uv_ref.at[mine(me)], UV.at[:, pl.ds(pl.multiple_of(z * rows_v, rows_v), rows_v), :], 9),
    ]
    def weight_part(buffer, rows, first, count, node):
        return buffer.at[pl.ds(first, count), pl.ds(pl.multiple_of(node * rows, rows), rows), :]

    splits = ((0, 2), (2, heads - 2))

    def key_copy(c, to):
        first, some = splits[c]
        src = uk_ref.at[pl.ds((2 * y + to % 2) * heads + first, some)]
        k = way(to)
        return remote(src, weight_part(UK, rows_k, first, some, z), wk_s.at[c, k], wk_r.at[c, k], {"node": to})

    def send_keys(c, to):
        copy = key_copy(c, to)
        copy.start()
        sends.append(copy)

    known = z + 2 * y + hd % 2 + hd // 2

    @pl.when(known > 0)
    def _():
        pl.semaphore_wait(barrier, known)

    for k in range(1, nodes):
        tell(ready.at[k], z >= k, {"node": (z + nodes - k) % nodes})
    for first_in, at, to in others:
        tell(ready.at[at], jnp.logical_not(first_in), to)

    def meet(condition, at):
        @pl.when(condition)
        def _():
            pl.semaphore_wait(ready.at[at], 1)

    def meet_node(to):
        meet(to > z, way(to))

    def meet_other(i):
        meet(others[i][0], others[i][1])

    opening = key_copy(0, inside)
    sends.append(opening)
    pl.when(inside < z)(opening.start)

    for copy in early:
        copy.wait()

    lane = lax.broadcasted_iota(jnp.int32, (1, 128), 1) % (ROPE // 2)
    freq = jnp.exp(lane.astype(jnp.float32) * (-2.0 * math.log(10000.0) / ROPE))

    def angles(first, count):
        at = (first + lax.broadcasted_iota(jnp.int32, (count, 128), 0)).astype(jnp.float32)
        turn = at * freq
        return jnp.cos(turn), jnp.sin(turn)

    raw = KV[...].astype(jnp.float32)
    latent = raw[:, :LATENT]
    mean = jnp.sum(latent * latent, axis=-1, keepdims=True) * (1.0 / LATENT)
    normed = latent * lax.rsqrt(mean + 1e-06) * gain_ref[...]
    rot = raw[:, LATENT:]
    swapped = jnp.concatenate([-rot[:, ROPE // 2:], rot[:, :ROPE // 2]], axis=-1)
    cosine, sine = angles(len_ref[z] + hd * part, part)
    rotary = rot * cosine[:, :ROPE] + swapped * sine[:, :ROPE]
    KB[me, nodes, quarter, :] = jnp.concatenate([normed, rotary], axis=-1).astype(jnp.bfloat16)

    column = lax.broadcasted_iota(jnp.int32, (8, old), 1)
    for i in range(2):
        session = 2 * p + i
        seen = column < 0
        for j in range(hits):
            place = column - (pages_ref[session, j] // owned) * BLOCK
            limit = jnp.minimum(len_ref[session] - j * BLOCK, BLOCK)
            seen = seen | ((place >= 0) & (place < limit))
        SEEN[2 * y + i] = jnp.where(seen, 1.0, 0.0)

    wide = 4 * heads * ROPE
    first = (lax.broadcasted_iota(jnp.int32, (NEW, wide), 1) % ROPE) < ROPE // 2
    cosine, sine = (jnp.concatenate([t] * (wide // 128), axis=1) for t in angles(len_ref[z], NEW))
    x = QR[...].astype(jnp.float32)
    ahead = pltpu.roll(x, wide - ROPE // 2, 1)
    behind = pltpu.roll(x, ROPE // 2, 1)
    QT[...] = (x * cosine + jnp.where(first, -ahead, behind) * sine).astype(jnp.bfloat16)

    load.wait()

    def local_page(session):
        found = jnp.int32(0)
        for j in range(hits):
            page = pages_ref[session, j] - z * owned
            found = jnp.where((page >= 0) & (page < owned), page, found)
        return found

    for n in range(nodes):
        PAY[n] = CB[local_page(n), quarter, :]
    for i in range(2):
        KB[2 * y + i, z, quarter, :] = CB[local_page(2 * p + i), quarter, :]

    def pages_at(group, owner):
        return KB.at[pl.ds(2 * group, 2), owner, quarter, :]

    def new_at(who):
        return KB.at[who, nodes, quarter, :]

    count = heads // phases

    def spread_part(group, origin, head):
        return KB.at[pl.ds(2 * group, 2), origin, rows_of(head), :]

    def fresh_part(head):
        return KB.at[:, nodes, rows_of(head), :]

    def spread(block, m):
        go(block, block, x_s.at[m], x_r.at[m], {"head": across})
        go(block, block, d_s.at[m], d_r.at[m], {"head": near})

    def relay(block, m):
        arrive(block, x_s.at[m], x_r.at[m], {"head": across})
        go(block, block, g_s.at[m], g_r.at[m], {"head": near})

    def send_queries(d):
        who, to = team[d]
        go(QT.at[:, cols_of(who, ROPE)], QP.at[me], t_s.at[d], t_r.at[d], to)
        go(qn_ref.at[:, cols_of(who, NOPE)], Q.at[me], q_s.at[d], q_r.at[d], to)

    def page_copy(to):
        k = way(to)
        return remote(PAY.at[pl.ds((to // 2) * 2, 2)], pages_at(y, z), e_s.at[k], e_r.at[k], {"node": to})

    def send_new(d):
        go(new_at(me), new_at(me), n_s.at[d], n_r.at[d], team[d][1])

    copies = [page_copy(to) for to in peers]
    sends.extend(copies)
    pl.when(outside < z)(copies[2].start)
    meet_node(inside)
    copies[1].start()
    meet_node(mate)
    copies[0].start()
    send_new(0)
    pl.when(inside > z)(opening.start)

    def go_when(condition, copy):
        pl.when(condition)(copy.start)
        relayed.append((condition, copy))

    send_keys(1, inside)
    send_keys(0, mate)
    send_keys(1, mate)
    final_keys = [key_copy(c, outside) for c in range(2)]
    for copy in final_keys:
        go_when(inner & (outside < z), copy)
    meet_other(0)
    go(pages_at(y, z), pages_at(y, z), c_s.at[0], c_r.at[0], {"grp": 1 - y})
    send_new(1)
    go(SEEN.at[ours], SEEN.at[ours], m_s.at[0], m_r.at[0], {"grp": 1 - y})
    meet_other(1)
    send_new(2)
    def key_block(c, node):
        return weight_part(UK, rows_k, *splits[c], node)

    def value_block(f, node):
        return weight_part(UV, rows_v, f * count, count, node)

    def value_copy(f, to):
        k = way(to)
        src = uv_ref.at[pl.ds((2 * y + to % 2) * heads + f * count, count)]
        return remote(src, value_block(f, z), wv_s.at[f, k], wv_r.at[f, k], {"node": to})

    def send_values(f, to):
        copy = value_copy(f, to)
        copy.start()
        sends.append(copy)

    meet_other(2)
    meet_other(3)
    spread(pages_at(y, z), 0)
    meet_node(outside)
    pl.when(outside > z)(copies[2].start)
    go(new_at(me), new_at(4), n_s.at[3], n_r.at[3], {"node": after})
    send_queries(0)
    send_queries(2)
    for copy in final_keys:
        go_when(inner & (outside > z), copy)

    QP[me] = QT[:, cols_of(me, ROPE)]
    for origin in peers:
        k = road(origin)
        block = pages_at(y, origin)
        arrive(block, e_s.at[k], e_r.at[k], {"node": origin})
        go(block, block, c_s.at[k], c_r.at[k], {"grp": 1 - y})
        spread(block, k)
    send_queries(1)
    mated, hop = road(mate), (outside - mate + nodes) % nodes

    def arrive_keys(c, origin):
        k = road(origin)
        block = key_block(c, origin)
        arrive(block, wk_s.at[c, k], wk_r.at[c, k], {"node": origin})

    def arrive_values(f, origin):
        k = road(origin)
        block = value_block(f, origin)
        arrive(block, wv_s.at[f, k], wv_r.at[f, k], {"node": origin})

    for c in range(2):
        pl.when(inner)(functools.partial(arrive_keys, c, mate))
        block = key_block(c, mate)
        go_when(inner, remote(block, block, fk_s.at[c], wk_r.at[c, hop], {"node": outside}))
    send_values(0, mate)
    send_values(1, mate)
    send_values(2, mate)
    send_values(3, mate)
    go_when(inner, value_copy(0, outside))
    send_values(0, inside)
    go_when(inner, value_copy(1, outside))
    send_values(1, inside)
    for origin in (z, *peers):
        k = road(origin)
        block = pages_at(1 - y, origin)
        arrive(block, c_s.at[k], c_r.at[k], {"grp": 1 - y})
        spread(block, nodes + k)
    for d, (who, to) in enumerate(team):
        arrive(new_at(who), n_s.at[d], n_r.at[d], to)
    arrive(new_at(4), n_s.at[3], n_r.at[3], {"node": back})
    spread(fresh_part(hd), 2 * nodes)
    far = near + 2 - 4 * (near // 2)
    for group in range(2):
        for origin in (z, *peers):
            relay(spread_part(y if group == 0 else 1 - y, origin, across), group * nodes + road(origin))
    relay(fresh_part(across), 2 * nodes)
    for head, r in ((near, d_r), (far, g_r)):
        for group in range(2):
            for origin in (z, *peers):
                m = group * nodes + road(origin)
                arrive(spread_part(y if group == 0 else 1 - y, origin, head), d_s.at[m], r.at[m], {"head": near})
        arrive(fresh_part(head), d_s.at[2 * nodes], r.at[2 * nodes], {"head": near})

    arrived = KB[4, nodes]
    slot = slot_ref[0, back] - z * owned

    def place(n, carry):
        CB[n] = jnp.where(slot == n, arrived, CB[n])
        return carry

    lax.fori_loop(0, owned, place, 0)

    arrive(SEEN.at[pl.ds(2 * (1 - y), 2)], m_s.at[0], m_r.at[0], {"grp": 1 - y})
    for copy in late:
        copy.wait()
    for d, (who, to) in enumerate(team):
        arrive(QP.at[who], t_s.at[d], t_r.at[d], to)
        arrive(Q.at[who], q_s.at[d], q_r.at[d], to)
    for f in (0, 1):
        pl.when(inner)(functools.partial(arrive_values, f, mate))
        block = value_block(f, mate)
        go_when(inner, remote(block, block, fv_s.at[f], wv_r.at[f, hop], {"node": outside}))
    go_when(inner, value_copy(2, outside))
    send_values(2, inside)
    go_when(inner, value_copy(3, outside))
    send_values(3, inside)
    for f in (2, 3):
        pl.when(inner)(functools.partial(arrive_values, f, mate))
        block = value_block(f, mate)
        go_when(inner, remote(block, block, fv_s.at[f], wv_r.at[f, hop], {"node": outside}))
    for c in range(2):
        pl.when(outer)(functools.partial(arrive_keys, c, mate))
        for origin in (inside, outside):
            arrive_keys(c, origin)

    for h in range(heads):
        QL[h] = jnp.dot(
            Q[:, :, h * NOPE:(h + 1) * NOPE].reshape(4 * NEW, NOPE), UK[h], preferred_element_type=jnp.float32
        ).astype(jnp.bfloat16)

    contract_last = (((1,), (1,)), ((), ()))
    causal = lax.broadcasted_iota(jnp.int32, (NEW, NEW), 1) <= lax.broadcasted_iota(jnp.int32, (NEW, NEW), 0)
    causal = jnp.where(causal, 1.0, 0.0)
    for i in range(4):
        seen = jnp.concatenate([jnp.broadcast_to(SEEN[i, 0:1, :], (NEW, old)), causal], axis=1) > 0.5
        keys = KB[i].reshape(total, LATENT + ROPE)
        key_latent = keys[:, :LATENT]
        tokens = slice(i * NEW, (i + 1) * NEW)
        q_part = QL[:, tokens, :].reshape(heads * NEW, LATENT)
        r_part = jnp.concatenate([QP[i, :, h * ROPE:(h + 1) * ROPE] for h in range(heads)], axis=0)
        scores = lax.dot_general(q_part, key_latent, contract_last, preferred_element_type=jnp.float32)
        scores = scores + lax.dot_general(r_part, keys[:, LATENT:], contract_last, preferred_element_type=jnp.float32)
        scores = (scores * score_scale).reshape(heads, NEW, total)
        scores = jnp.where(seen[None], scores, -1e30)
        row_max = jnp.max(scores, axis=-1, keepdims=True)
        terms = jnp.where(seen[None], jnp.exp(scores - row_max), 0.0)
        weights = (terms / jnp.sum(terms, axis=-1, keepdims=True)).astype(jnp.bfloat16)
        mixed = jnp.dot(
            weights.reshape(heads * NEW, total), key_latent, preferred_element_type=jnp.float32
        ).astype(jnp.bfloat16)
        LAT[:, tokens, :] = mixed.reshape(heads, NEW, LATENT)

    def result_part(who, f):
        return attn_ref.at[:, pl.ds(pl.multiple_of((who * heads + f * count) * VHEAD, 128), count * VHEAD)]

    for f in range(phases):
        pl.when(outer)(functools.partial(arrive_values, f, mate))
        for origin in (inside, outside):
            arrive_values(f, origin)
        for h in range(f * count, (f + 1) * count):
            OUT[:, :, h * VHEAD:(h + 1) * VHEAD] = jnp.dot(
                LAT[h], UV[h], preferred_element_type=jnp.float32
            ).astype(jnp.bfloat16).reshape(4, NEW, VHEAD)
        here = pl.ds(f * count * VHEAD, count * VHEAD)
        for d in (2, 0, 1):
            who, to = team[d]
            go(OUT.at[who, :, here], result_part(me, f), o_s.at[f, d], o_r.at[f, d], to)
    attn_ref[:, cols_of(me, VHEAD)] = OUT[me]
    for f in range(phases):
        for d, (who, to) in enumerate(team):
            arrive(result_part(who, f), o_s.at[f, d], o_r.at[f, d], to)
    for copy in sends:
        copy.wait_send()
    for condition, copy in relayed:
        pl.when(condition)(copy.wait_send)


def write_kernel(attn_ref, pages_ref, attn_out, pages_out, done):
    copies = [
        pltpu.make_async_copy(attn_ref, attn_out, done.at[0]),
        pltpu.make_async_copy(pages_ref, pages_out, done.at[1]),
    ]
    for copy in copies:
        copy.start()
    for copy in copies:
        copy.wait()


def fused_device(q_nope, q_rope, kv_new, kv_gain, cache, w_uk, w_uv, hit_pages, hit_len, page_slots):
    nodes = lax.axis_size("node")
    width = LATENT + ROPE
    heads = w_uk.shape[0] // 4
    phases = PHASES if heads % PHASES == 0 else 1
    vmem = pl.BlockSpec(memory_space=pltpu.VMEM)
    anywhere = pl.BlockSpec(memory_space=pl.ANY)
    bf16 = jnp.bfloat16
    dma = pltpu.SemaphoreType.DMA

    def pair(*shape):
        return [dma(shape), dma(shape)]

    attn, pages = pl.pallas_call(
        functools.partial(fused_kernel, nodes, phases, 1.0 / math.sqrt(NOPE + ROPE)),
        name="fused",
        out_shape=(
            pltpu.VMEM((NEW, 4 * heads * VHEAD), bf16),
            pltpu.VMEM(cache.shape, bf16),
        ),
        in_specs=[anywhere] * 10,
        out_specs=(vmem, vmem),
        scratch_shapes=[
            pltpu.VMEM((heads, NOPE, LATENT), bf16),
            pltpu.VMEM((heads, LATENT, VHEAD), bf16),
            pltpu.VMEM((5, nodes + 1, BLOCK, width), bf16),
            pltpu.VMEM((nodes, BLOCK // 4, width), bf16),
            pltpu.VMEM((BLOCK // 4, width), bf16),
            pltpu.VMEM((4, NEW, heads * NOPE), bf16),
            pltpu.VMEM((NEW, 4 * heads * ROPE), bf16),
            pltpu.VMEM((NEW, 4 * heads * ROPE), bf16),
            pltpu.VMEM((4, NEW, heads * ROPE), bf16),
            pltpu.VMEM((heads, 4 * NEW, LATENT), bf16),
            pltpu.VMEM((heads, 4 * NEW, LATENT), bf16),
            pltpu.VMEM((4, NEW, heads * VHEAD), bf16),
            pltpu.VMEM((4, 8, nodes * BLOCK), jnp.float32),
            pltpu.SMEM(hit_pages.shape, jnp.int32),
            pltpu.SMEM(hit_len.shape, jnp.int32),
            pltpu.SMEM(page_slots.shape[::-1], jnp.int32),
            pltpu.VMEM((1, LATENT), jnp.float32),
            dma((10,)),
            *pair(nodes), *pair(nodes), *pair(4), *pair(3), *pair(3), *pair(1),
            *pair(2 * nodes + 1), *pair(2 * nodes + 1), *pair(2 * nodes + 1), *pair(2, nodes), *pair(phases, nodes), dma((2,)), dma((phases,)), *pair(phases, 3),
            pltpu.SemaphoreType.REGULAR((nodes + 4,)),
        ],
        compiler_params=pltpu.CompilerParams(
            collective_id=0, has_side_effects=True, vmem_limit_bytes=60 << 20
        ),
    )(hit_pages, hit_len, page_slots.T, kv_gain[None, :], q_nope, q_rope, kv_new, cache, w_uk, w_uv)
    return pl.pallas_call(
        write_kernel,
        name="write",
        out_shape=(
            jax.ShapeDtypeStruct(attn.shape, bf16),
            jax.ShapeDtypeStruct(cache.shape, bf16),
        ),
        in_specs=[vmem, vmem],
        out_specs=(anywhere, anywhere),
        scratch_shapes=[dma((2,))],
    )(*(pltpu.with_memory_space_constraint(x, pltpu.VMEM) for x in (attn, pages)))


def choose(*operands):
    w_uk, w_uv = operands[5], operands[6]
    nodes, grps, fan = (lax.axis_size(name) for name in ("node", "grp", "head"))
    fits = (
        (nodes, grps, fan) == (4, 2, 4)
        and NEW == BLOCK
        and w_uk.shape[0] % 8 == 0
        and w_uk.shape[1] % 16 == 0
        and w_uv.shape[1] % 16 == 0
    )
    return (fused_device if fits else per_device)(*operands)


def solution(mesh):
    placed = (
        P(("grp", "node"), "head"),
        P(("grp", "node"), "head"),
        P(("grp", "node"), None),
        P(),
        P(("grp", "node"), None, None),
        P("head", "node", None),
        P("head", "node", None),
        P("grp", None),
        P("grp"),
        P("grp", None),
    )
    return jax.shard_map(
        choose,
        mesh=mesh,
        in_specs=placed,
        out_specs=(P(("grp", "node"), "head"), P(("grp", "node"), None, None)),
        check_vma=False,
    )
```
